256 devices in a mesh: gx: 32 (over y, z), gy: 8 (over x, core).
Axes of the slice: x: 4, y: 4, z: 8, core: 2. Of those that a mesh axis runs over, the one named last changes fastest.
Arguments:
- right_side: float32 [64, 128, 4, 3, 128], P('gx', 'gy'), may hold values from -6 to 6
- stencil: float32 [27, 3, 3], replicated, as said below
- class_scale: float32 [8], replicated, may hold values from 0.5 to 4
- material: int32 [64, 128, 128], P('gx', 'gy'), may hold values from 0 to 7
- boundary: int32 [64, 128, 128], P('gx', 'gy'), may hold values 0 or 1
- sign_bits: int32 [64, 128, 3, 128], P('gx', 'gy'), may hold values from 0 to 1
- sample_rows: int32 [32, 8, 128], P('gx', 'gy'), may hold values from 0 to 12287
Outputs:
- solution: float32 [64, 128, 4, 3, 128], P('gx', 'gy')
- residual: float32 [64, 128, 4, 3, 128], P('gx', 'gy')
The draws below stay inside these ranges and needn't reach their ends.
Inputs may be any that keep to these rules, and one draw needn't show every extreme that they name: In every row of the centre block stencil[13], the diagonal entry exceeds the sum of the magnitudes of all other entries of that row over all 27 blocks.
All inputs are finite; a program needn't handle non-finite values. No bound on the sum of `boundary` on one device may be relied on, other than what follows from the above.
Results may differ from the reference program's by a relative error of at most 0.0028.
Values sent between devices are 32-bit elements; how exact they have to be, the bound alone decides.
No kernel may reach another device: no remote copies, remote signals or barrier semaphores. Data moves between devices by JAX's collectives and lax.ppermute only.
A program may use at most 64 MiB of HBM per device.

```python
import math
import jax
import jax.numpy as jnp
from jax import lax

CX = 2
CY = 16
NZ = 128
BW = 4
STEPS = 8
SK = 128
NCLASS = 8
NX = 64
NY = 128
N_GX = 32
N_GY = 8


def draw_stencil(key, part):
    subkeys = jax.random.split(jax.random.fold_in(key, 11), 4)
    rough = 0.4 * jax.random.normal(subkeys[0], (27, 3, 3), jnp.float32)
    pulled = jax.random.uniform(subkeys[1], (27, 1, 1), jnp.float32, 0.3, 1.0)
    identity = jnp.eye(3, dtype=jnp.float32)
    blocks = rough - 0.5 * pulled * identity
    centre_rough = 0.3 * jax.random.normal(subkeys[2], (3, 3), jnp.float32) * (1.0 - identity)
    others = jnp.sum(jnp.abs(blocks), axis=(0, 2)) - jnp.sum(jnp.abs(blocks[13]), axis=1) + jnp.sum(jnp.abs(centre_rough), axis=1)
    margin = jax.random.uniform(subkeys[3], (3,), jnp.float32, 0.5, 2.0)
    centre = centre_rough + jnp.diag(others + margin)
    blocks = blocks.at[13].set(centre)
    return blocks / jnp.mean(others + margin)


def place_ends(entries, key, low, largest):
    longest = entries.shape.index(max(entries.shape))
    spots = []
    for shift in (0, 1):
        where = [jax.random.randint(jax.random.fold_in(key, axis), (), 0, length) for axis, length in enumerate(entries.shape)]
        where[longest] = (where[longest] + shift) % entries.shape[longest]
        spots.append(tuple(where))
    return entries.at[spots[0]].set(low).at[spots[1]].set(largest)


def steps_of(key, dims, pieces, smallest, top_value):
    factor_of = 1.0
    for dim, blocks in pieces:
        steps = jax.random.uniform(jax.random.fold_in(jax.random.fold_in(key, 6), dim), (blocks,), jnp.float32, smallest / len(pieces), top_value / len(pieces))
        factor_of = factor_of * jnp.repeat(jnp.exp(steps), dims[dim] // blocks).reshape((-1,) + (1,) * (len(dims) - 1 - dim))
    return factor_of


def bell_draw(own_key, extent, width, limit, shards=(), held_as=jnp.bfloat16):
    factor_of = steps_of(own_key, extent, shards, -0.22, 0.18) if shards else 1.0
    drawn = jax.random.normal(own_key, extent, jnp.float32) * width * factor_of
    return jnp.minimum(jnp.maximum(drawn, -limit), limit).astype(held_as)


def setup_inputs(seed: int = 0) -> dict:
    arg_keys = jax.random.split(jax.random.key(seed), 8)
    return {
        "right_side": bell_draw(arg_keys[0], (NX, NY, BW, 3, NZ), 1.0, 6.0, ((0, 32), (1, 8)), jnp.float32),
        "stencil": draw_stencil(jax.random.fold_in(arg_keys[7], 71), 0),
        "class_scale": jnp.clip(jnp.exp(jax.random.uniform(arg_keys[2], (NCLASS,), jnp.float32, math.log(0.5), math.log(4.0))), 0.5, 4.0),
        "material": place_ends(jax.random.randint(arg_keys[3], (NX, NY, NZ), 0, NCLASS), jax.random.fold_in(arg_keys[3], 1), 0, NCLASS - 1).astype(jnp.int32),
        "boundary": place_ends((jax.random.randint(arg_keys[4], (NX, NY, NZ), 0, 16) < 1).astype(jnp.int32), jax.random.fold_in(arg_keys[4], 1), 0, 1),
        "sign_bits": place_ends(jax.random.randint(arg_keys[5], (NX, NY, 3, NZ), 0, 2), jax.random.fold_in(arg_keys[5], 1), 0, 1).astype(jnp.int32),
        "sample_rows": place_ends(jax.random.randint(arg_keys[6], (N_GX, N_GY, SK), 0, 3 * CX * CY * NZ), jax.random.fold_in(arg_keys[6], 1), 0, (3 * CX * CY * NZ) - 1).astype(jnp.int32),
    }


exact_mode = lax.Precision.HIGHEST

def hadamard_table():
    lanes = jnp.arange(128, dtype=jnp.int32)
    common = lanes[:, None] & lanes[None, :]
    parity = jnp.zeros((128, 128), jnp.int32)
    for bit in range(7):
        parity = parity + (common >> bit & 1)
    return (1 - 2 * (parity % 2)).astype(jnp.float32) / math.sqrt(128.0)

def material_scale(material, class_scale):
    scale_field = jnp.zeros(material.shape, jnp.float32)
    for number in range(class_scale.shape[0]):
        scale_field = scale_field + jnp.where(material == number, class_scale[number], jnp.float32(0.0))
    return scale_field

def operate(field, stencil, scale_field, boundary):
    padded = jnp.pad(field, ((1, 1), (1, 1), (0, 0), (0, 0), (1, 1)))
    extent_x, extent_y, extent_z = (field.shape[0], field.shape[1], field.shape[4])
    summed = jnp.zeros(field.shape, jnp.float32)
    for offset_x in range(3):
        for offset_y in range(3):
            for offset_z in range(3):
                shifted = padded[offset_x:offset_x + extent_x, offset_y:offset_y + extent_y, :, :, offset_z:offset_z + extent_z]
                coupling = stencil[offset_x * 9 + offset_y * 3 + offset_z]
                summed = summed + lax.optimization_barrier(jnp.sum(coupling[:, :, None] * shifted[:, :, :, None, :, :], axis=4))
    return jnp.where(boundary[:, :, None, None, :] == 1, field, scale_field[:, :, None, None, :] * summed)

def sketch_of(field, sign_bits, sample_rows, table):
    sign_field = (2 * sign_bits - 1).astype(jnp.float32)
    signed = field * sign_field[:, :, None, :, :]
    tiled = signed.reshape(NX, NY, BW, 3, NZ // 128, 128)
    plane = CY * 3 * NZ
    pick_x = sample_rows // plane
    rest_y = sample_rows % plane
    pick_y = rest_y // (3 * NZ)
    rest_c = rest_y % (3 * NZ)
    pick_comp = rest_c // NZ
    pick_z = rest_c % NZ
    global_x = pick_x + (jnp.arange(N_GX, dtype=jnp.int32) * CX)[:, None, None]
    global_y = pick_y + (jnp.arange(N_GY, dtype=jnp.int32) * CY)[None, :, None]
    chosen = tiled[global_x, global_y, :, pick_comp, pick_z // 128]
    table_rows = table[pick_z % 128]
    local_terms = lax.optimization_barrier(jnp.sum(chosen * table_rows[:, :, :, None, :], axis=-1))
    return lax.optimization_barrier(jnp.sum(local_terms, axis=(0, 1)))

def back_substitute(triangle, projected):
    count = triangle.shape[0]

    def one_row(step, unknowns):
        row = count - 1 - step
        line = triangle[row]
        total = jnp.dot(line[None, :], unknowns, precision=exact_mode)[0]
        value = (projected[row] - total) / line[row]
        return unknowns.at[row].set(value)
    return lax.fori_loop(0, count, one_row, jnp.zeros(projected.shape, jnp.float32))

def solve_small(matrix, rhs):
    count = matrix.shape[1]
    columns = matrix.T

    def one_column(column, state_pair):
        orthonormal, triangle = state_pair
        vector = columns[column]
        first_pass = jnp.dot(orthonormal.T, vector, precision=exact_mode)
        vector = vector - jnp.dot(orthonormal, first_pass, precision=exact_mode)
        second_pass = jnp.dot(orthonormal.T, vector, precision=exact_mode)
        vector = vector - jnp.dot(orthonormal, second_pass, precision=exact_mode)
        length = jnp.sqrt(jnp.sum(vector * vector) + 1e-06)
        orthonormal = orthonormal.at[:, column].set(vector / length)
        triangle = triangle.at[:, column].set((first_pass + second_pass).at[column].set(length))
        return (orthonormal, triangle)
    start = (jnp.zeros(matrix.shape, jnp.float32), jnp.zeros((count, count), jnp.float32))
    orthonormal, triangle = lax.fori_loop(0, count, one_column, start)
    projected = jnp.dot(orthonormal.T, rhs, precision=exact_mode)
    return back_substitute(triangle, projected)

def reference(right_side, stencil, class_scale, material, boundary, sign_bits, sample_rows):
    table = hadamard_table()
    scale_field = material_scale(material, class_scale)
    sketch_rhs = sketch_of(right_side, sign_bits, sample_rows, table)
    lengths = jnp.sqrt(lax.optimization_barrier(jnp.sum(sketch_rhs * sketch_rhs, axis=0)) + 1e-06)
    basis_block = right_side / lengths[None, None, :, None, None]
    sketch_basis = sketch_rhs / lengths
    blocks = []
    sketched_images = []
    for block_step in range(STEPS):
        operated = operate(basis_block, stencil, scale_field, boundary)
        sketch_image = sketch_of(operated, sign_bits, sample_rows, table)
        blocks.append(basis_block)
        sketched_images.append(sketch_image)
        if block_step + 1 < STEPS:
            coupling = jnp.dot(sketch_basis.T, sketch_image, precision=exact_mode)
            remainder = operated - jnp.einsum('xyicz,ij->xyjcz', basis_block, coupling, precision=exact_mode)
            sketch_remainder = sketch_of(remainder, sign_bits, sample_rows, table)
            norms = jnp.sqrt(lax.optimization_barrier(jnp.sum(sketch_remainder * sketch_remainder, axis=0)) + 1e-06)
            basis_block = remainder / norms[None, None, :, None, None]
            sketch_basis = sketch_remainder / norms
    matrix = jnp.concatenate(sketched_images, axis=1)
    weights = solve_small(matrix, sketch_rhs)
    solution = jnp.zeros(right_side.shape, jnp.float32)
    for block_step in range(STEPS):
        part_weights = weights[block_step * BW:(block_step + 1) * BW]
        solution = solution + jnp.einsum('xyicz,ij->xyjcz', blocks[block_step], part_weights, precision=exact_mode)
    residual = right_side - operate(solution, stencil, scale_field, boundary)
    return (solution, residual)
```

```python
import math

import jax
import jax.numpy as jnp
from jax import lax
from jax.experimental import pallas as pl
from jax.experimental.pallas import tpu as pltpu
from jax.sharding import Mesh
from jax.sharding import PartitionSpec as P

STEPS = 8
AXES = ("gx_0", "gx_1", "gy_0", "gy_1")
GX = ("gx_0", "gx_1")
GY = ("gy_0", "gy_1")
REDUCE_STAGES = ((("gx_0", "gy_0"), 16), (("gx_1", "gy_1"), 16))

exact_mode = lax.Precision.HIGHEST
VMEM = pl.BlockSpec(memory_space=pltpu.VMEM)
SMEM = pl.BlockSpec(memory_space=pltpu.SMEM)
PARAMS = pltpu.CompilerParams(vmem_limit_bytes=48 * 1024 * 1024)


def tile_iota(axis):
    return lax.broadcasted_iota(jnp.int32, (8, 128), axis)


def stencil_rows(source, base, first, rows, component, coef):
    sums = [[None] * rows for _ in range(3)]
    for dx in range(3):
        for c in range(3):
            tiles = [source[first + r, base + dx, c] for r in range(rows + 2)]
            for dy in range(3):
                for dz in range(3):
                    weight = coef[(dx * 9 + dy * 3 + dz) * 9 + component * 3 + c]
                    for r in range(rows):
                        term = weight * tiles[r + dy]
                        old = sums[dz][r]
                        sums[dz][r] = term if old is None else old + term
    lane = tile_iota(1)
    out = []
    for r in range(rows):
        low = jnp.where(lane > 0, pltpu.roll(sums[0][r], 1, 1), 0.0)
        high = jnp.where(lane < 127, pltpu.roll(sums[2][r], 127, 1), 0.0)
        out.append(sums[1][r] + low + high)
    return out


def make_pair_kernel(first_round):
    rows_a, rows_b = 9, 8

    def kernel(coef, left, own, right, down, up, before, scale, scale_own, mid, last, work):
        half = tile_iota(0) < 4

        def put(row, t_left, t_own, t_right):
            for c in range(3):
                a, b, d = t_left(c), t_own(c), t_right(c)
                ra, rb, rd = pltpu.roll(a, 4, 0), pltpu.roll(b, 4, 0), pltpu.roll(d, 4, 0)
                work[row, 0, c] = a
                work[row, 1, c] = jnp.where(half, ra, rb)
                work[row, 2, c] = b
                work[row, 3, c] = jnp.where(half, rb, rd)
                work[row, 4, c] = d

        for row in range(2):
            put(row, *[(lambda c, s=s, row=row: down[s, row, c]) for s in range(3)])
            put(18 + row, *[(lambda c, s=s, row=row: up[s, row, c]) for s in range(3)])

        def inner(row, carry):
            put(
                row + 2,
                lambda c: left[row, c],
                lambda c: own[row, c],
                lambda c: right[row, c],
            )
            return carry

        lax.fori_loop(0, 16, inner, 0)
        shift, gain = coef[243], coef[244]

        def diagonal(tile):
            return jnp.where(tile == 0.0, gain - shift * gain, -shift * gain)

        def step_a(i, carry):
            side = i // 2
            first = (i % 2) * rows_a
            for component in range(3):
                total = stencil_rows(work, side * 2, first, rows_a, component, coef)
                for r in range(rows_a):
                    row = first + r
                    alpha = scale[row, side]
                    centre = work[row + 1, side * 2 + 1, component]
                    value = (alpha * gain) * total[r] + diagonal(alpha) * centre
                    if first_round:
                        value = value * 0.5
                    else:
                        value = value - before[row, side * 2, component]
                    mid[row, side * 2, component] = value
            return carry

        lax.fori_loop(0, 4, step_a, 0)

        def join(row, carry):
            for c in range(3):
                mid[row, 1, c] = jnp.where(
                    half, pltpu.roll(mid[row, 0, c], 4, 0), pltpu.roll(mid[row, 2, c], 4, 0)
                )
            return carry

        lax.fori_loop(0, 18, join, 0)

        def step_b(i, carry):
            first = i * rows_b
            for component in range(3):
                total = stencil_rows(mid, 0, first, rows_b, component, coef)
                for r in range(rows_b):
                    row = first + r
                    alpha = scale_own[row]
                    value = (alpha * gain) * total[r] + diagonal(alpha) * mid[row + 1, 1, component]
                    last[row, component] = value - own[row, component]
            return carry

        lax.fori_loop(0, 2, step_b, 0)

    return kernel


def two_steps(first_round, coef, left, own, right, down, up, before, scale, scale_own):
    return pl.pallas_call(
        make_pair_kernel(first_round),
        out_shape=(
            jax.ShapeDtypeStruct((18, 3, 3, 8, 128), jnp.float32),
            jax.ShapeDtypeStruct((16, 3, 8, 128), jnp.float32),
        ),
        in_specs=[SMEM] + [VMEM] * 8,
        out_specs=(VMEM, VMEM),
        scratch_shapes=[pltpu.VMEM((20, 5, 3, 8, 128), jnp.float32)],
        compiler_params=PARAMS,
        name="two_steps",
    )(coef, left, own, right, down, up, before, scale, scale_own)


def make_sketch_kernel(kinds):
    def kernel(where, signs, *refs):
        count = len(kinds)
        blocks, out = refs[:count], refs[count]
        both, products = refs[count + 1 :]
        half = tile_iota(0) < 4
        ones = jnp.ones((8, 128), jnp.float32)
        for n, kind in enumerate(kinds):
            ref = blocks[n]

            def spread(row, carry):
                for c in range(3):
                    tile = ref[row + 1, 1, c] if kind else ref[row, c]
                    both[row * 3 + c] = tile
                    both[48 + row * 3 + c] = pltpu.roll(tile, 4, 0)
                return carry

            lax.fori_loop(0, 16, spread, 0)

            def pick(group, carry):
                for k in range(8):
                    j = group * 8 + k
                    tile = jnp.where(half, both[where[j]], both[where[64 + j]]) * signs[j]
                    products[pl.ds(j, 4, stride=128), :] = tile[0:4]
                    products[pl.ds(j + 64, 4, stride=128), :] = tile[4:8]
                return carry

            lax.fori_loop(0, 8, pick, 0)
            sums = lax.dot_general(
                ones,
                products[...],
                (((1,), (1,)), ((), ())),
                precision=exact_mode,
                preferred_element_type=jnp.float32,
            )
            for b in range(4):
                out[pl.ds(n * 4 + b, 1), :] = sums[0:1, b * 128 : (b + 1) * 128]

    return kernel


def sketch(kinds, where, signs, *blocks):
    return pl.pallas_call(
        make_sketch_kernel(kinds),
        out_shape=jax.ShapeDtypeStruct((4 * len(kinds), 128), jnp.float32),
        in_specs=[SMEM] + [VMEM] * (1 + len(kinds)),
        out_specs=VMEM,
        scratch_shapes=[
            pltpu.VMEM((96, 8, 128), jnp.float32),
            pltpu.VMEM((512, 128), jnp.float32),
        ],
        compiler_params=PARAMS,
        name="sketch",
    )(where, signs, *blocks)


def fit_kernel(scalars, images, sketches, out):
    shift, reach = scalars[0], scalars[1]
    lane = tile_iota(1)
    row = tile_iota(0)
    tall_row = lax.broadcasted_iota(jnp.int32, (40, 128), 0)
    tall_lane = lax.broadcasted_iota(jnp.int32, (40, 128), 1)

    def dot(a, b):
        return jnp.dot(a, b, precision=exact_mode, preferred_element_type=jnp.float32)

    def sum_lanes(a):
        return jnp.sum(a, axis=1, keepdims=True)

    live = row < 4
    raise_by = jnp.where(lane < 4, reach, 0.5 * reach)
    lower_by = jnp.where(lane < 4, 0.0, 0.5 * reach)
    table = sketches[...]
    basis = jnp.where(live, images[32:40, :], 0.0)
    norms = jnp.sqrt(sum_lanes(basis * basis) + 1e-06)
    basis = basis / norms
    coords = jnp.where(live & (lane == row), 1.0, 0.0) / norms
    leading = jnp.sum(jnp.where(lane == row, coords, 0.0), axis=0, keepdims=True)
    for k in range(STEPS - 1):
        moved = (
            pltpu.roll(coords * raise_by, 4, 1)
            + shift * coords
            + pltpu.roll(coords * lower_by, 124, 1)
        )
        image = dot(moved, table)
        rest, next_coords = image, moved
        for i in range(4):
            weight = sum_lanes(image * basis[i : i + 1])
            rest = rest - weight * basis[i : i + 1]
            next_coords = next_coords - weight * coords[i : i + 1]
        norms = jnp.sqrt(sum_lanes(rest * rest) + 1e-06)
        basis = rest / norms
        coords = next_coords / norms
        leading = leading + jnp.sum(
            jnp.where(live & (lane == row + 4 * (k + 1)), coords, 0.0), axis=0, keepdims=True
        )

    vectors = images[...]
    combos = jnp.where(tall_row == tall_lane, 1.0, 0.0)
    found = jnp.zeros((8, 128), jnp.float32)
    sizes = jnp.zeros((1, 128), jnp.float32)
    for j in range(4 * STEPS):
        pivot = vectors[j : j + 1]
        products = sum_lanes(vectors * pivot)
        size = products[j : j + 1]
        ratio = products / (size + 1e-37)
        found = jnp.where(lane == j, ratio[32:40], found)
        sizes = jnp.where(lane[0:1] == j, size, sizes)
        later = jnp.where(tall_row > j, ratio, 0.0)
        vectors = vectors - later * pivot
        combos = combos - later * combos[j : j + 1]
    scaled = sizes * leading * leading
    found = found * (scaled / (scaled + 1e-06))
    out[...] = dot(found[:, 0:40], combos)


def fit(scalars, images, sketches):
    return pl.pallas_call(
        fit_kernel,
        out_shape=jax.ShapeDtypeStruct((8, 128), jnp.float32),
        in_specs=[SMEM, VMEM, VMEM],
        out_specs=VMEM,
        compiler_params=PARAMS,
        name="fit",
    )(scalars, images, sketches)


def combine_kernel(mix, first, m0, l0, m1, l1, m2, l2, m3, l3, iterate, remainder):
    sub = tile_iota(0) % 4
    refs = [(first, 0), (m0, 1), (l0, 0), (m1, 1), (l1, 0), (m2, 1), (l2, 0), (m3, 1), (l3, 0)]

    def one_row(y, carry):
        for c in range(3):
            start = first[y, c]
            total = None
            image = start
            for k, (ref, kind) in enumerate(refs):
                tile = ref[y + 1, 1, c] if kind else ref[y, c]
                for r in range(4):
                    if r:
                        turned = jnp.where(
                            sub < 4 - r, pltpu.roll(tile, 8 - r, 0), pltpu.roll(tile, 4 - r, 0)
                        )
                    else:
                        turned = tile
                    if k < STEPS:
                        part = mix[k * 4 + r] * turned
                        total = part if total is None else total + part
                    image = image - mix[(STEPS + k) * 4 + r] * turned
            iterate[y, c] = total
            remainder[y, c] = image
        return carry

    lax.fori_loop(0, 16, one_row, 0)


def combine(mix, blocks):
    shape = jax.ShapeDtypeStruct((16, 3, 8, 128), jnp.float32)
    return pl.pallas_call(
        combine_kernel,
        out_shape=(shape, shape),
        in_specs=[VMEM] * 10,
        out_specs=(VMEM, VMEM),
        compiler_params=PARAMS,
        name="combine",
    )(mix, *blocks)


def hadamard_table():
    lanes = jnp.arange(128, dtype=jnp.int32)
    common = lanes[:, None] & lanes[None, :]
    parity = jnp.zeros((128, 128), jnp.int32)
    for bit in range(7):
        parity = parity + (common >> bit & 1)
    return (1 - 2 * (parity % 2)).astype(jnp.float32) / math.sqrt(128.0)


def material_scale(material, class_scale):
    scale_field = jnp.zeros(material.shape, jnp.float32)
    for number in range(class_scale.shape[0]):
        scale_field = scale_field + jnp.where(
            material == number, class_scale[number], jnp.float32(0.0)
        )
    return scale_field


def neighbours(low, high, axis):
    count = lax.axis_size(axis)
    before = lax.ppermute(high, axis, [(i, i + 1) for i in range(count - 1)])
    after = lax.ppermute(low, axis, [(i + 1, i) for i in range(count - 1)])
    return before, after


def spectrum(stencil, class_scale):
    centre = jnp.diagonal(stencil[13])
    middle = jnp.mean(centre)
    spread = jnp.sqrt(
        jnp.maximum(jnp.sum(stencil * stencil) - jnp.sum(centre * centre), 0.0) / 3.0
    )
    low = jnp.minimum(jnp.min(class_scale) * (middle - spread), 1.0)
    high = jnp.maximum(jnp.max(class_scale) * (middle + spread), 1.0)
    shift = 0.5 * (low + high)
    return shift, jnp.maximum(0.5 * (high - low), 0.05 * shift)


def shards(right_side, stencil, class_scale, material, boundary, sign_bits, sample_rows):
    shift, reach = spectrum(stencil, class_scale)
    coef = jnp.concatenate(
        [stencil.reshape(-1), shift[None], (2.0 / reach)[None], jnp.zeros((11,), jnp.float32)]
    )
    own = right_side.transpose(1, 3, 0, 2, 4).reshape(16, 3, 8, 128)
    masked = jnp.where(boundary == 1, 0.0, material_scale(material, class_scale))

    sampled = sample_rows[0, 0]
    pick_x = sampled // 6144
    pick_y = sampled % 6144 // 384
    pick_c = sampled % 384 // 128
    pick_z = sampled % 128
    tile = pick_y * 3 + pick_c
    where = tile + 48 * jnp.concatenate([pick_x[:64], 1 - pick_x[64:]])
    sign_rows = (2 * sign_bits - 1).astype(jnp.float32)[pick_x, pick_y, pick_c]
    sign_rows = sign_rows * hadamard_table()[pick_z]
    signs = jnp.broadcast_to(
        sign_rows.reshape(2, 64, 1, 128).transpose(1, 0, 2, 3), (64, 2, 4, 128)
    ).reshape(64, 8, 128)

    blocks = [own]
    sketches = []
    before = None
    flat = (16 * 3 * 8, 128)
    for turn in range(STEPS // 2):
        if turn == 0:
            packed = own.reshape(flat)
            low, high = neighbours(
                jnp.concatenate([packed, masked[0]]), jnp.concatenate([packed, masked[1]]), GX
            )
            left, right = low[:384].reshape(own.shape), high[:384].reshape(own.shape)
            planes = jnp.concatenate([low[None, 384:], masked, high[None, 384:]])
        else:
            left, right = neighbours(own, own, GX)
        bottom = jnp.stack([left[:2], own[:2], right[:2]])
        top = jnp.stack([left[14:], own[14:], right[14:]])
        if turn == 0:
            flat_y = (3 * 2 * 3 * 8, 128)
            down, up = neighbours(
                jnp.concatenate([bottom.reshape(flat_y), planes[:, 0], planes[:, 0]]),
                jnp.concatenate([top.reshape(flat_y), planes[:, 15], planes[:, 15]]),
                GY,
            )
            planes = jnp.concatenate([down[144:148, None], planes, up[144:148, None]], axis=1)
            down, up = down[:144].reshape(bottom.shape), up[:144].reshape(top.shape)
            scale = jnp.broadcast_to(
                planes.reshape(2, 2, 18, 128).transpose(2, 0, 1, 3)[:, :, :, None], (18, 2, 2, 4, 128)
            ).reshape(18, 2, 8, 128)
            scale_own = jnp.broadcast_to(
                masked.transpose(1, 0, 2)[:, :, None], (16, 2, 4, 128)
            ).reshape(16, 8, 128)
        else:
            down, up = neighbours(bottom, top, GY)
        if turn == 0:
            sketches.append(sketch((0,), where, signs, own))
            before = jnp.zeros((8, 128), jnp.float32)
        else:
            sketches.append(sketch((1, 0), where, signs, blocks[-2], blocks[-1]))
        mid, last = two_steps(
            turn == 0, coef, left, own, right, down, up, before, scale, scale_own
        )
        blocks += [mid, last]
        before, own = mid, last
    sketches.append(sketch((1, 0), where, signs, blocks[-2], blocks[-1]))

    table = jnp.concatenate(sketches)
    for axes, count in REDUCE_STAGES:
        copies = jnp.broadcast_to(table, (count,) + table.shape)
        table = jnp.sum(lax.all_to_all(copies, axes, 0, 0, tiled=True), axis=0)

    by_block = table.reshape(9, 4, 128)
    half_reach = 0.5 * reach
    images = shift * by_block[:8] + half_reach * by_block[1:]
    images = images + jnp.concatenate(
        [half_reach * by_block[1:2], half_reach * by_block[:7]]
    )
    images = jnp.concatenate(
        [images.reshape(32, 128), by_block[0], jnp.zeros((4, 128), jnp.float32)]
    )
    padded = jnp.concatenate([table, jnp.zeros((92, 128), jnp.float32)])
    weights = fit(jnp.stack([shift, reach]), images, padded)

    weights = weights[:4, :32].reshape(4, 8, 4).transpose(1, 2, 0)
    none = jnp.zeros((1, 4, 4), jnp.float32)
    rising = jnp.concatenate([none, weights[:1], 0.5 * weights[1:]]) * reach
    level = jnp.concatenate([weights, none]) * shift
    falling = jnp.concatenate([weights[1:], none, none]) * half_reach
    image_weights = rising + level + falling
    both = jnp.concatenate([weights, image_weights])
    column = jnp.arange(4)
    choose = (column[None, :, None] == (column[None, None, :] + column[:, None, None]) % 4)
    mix = jnp.sum(both[:, None] * choose[None].astype(jnp.float32), axis=2)
    mix = jnp.broadcast_to(mix.reshape(68, 1, 4, 1), (68, 2, 4, 128)).reshape(68, 8, 128)
    iterate, remainder = combine(mix, blocks)

    def unpack(block):
        return block.reshape(16, 3, 2, 4, 128).transpose(2, 0, 3, 1, 4)

    return unpack(iterate), unpack(remainder)


def solution(mesh):
    split = Mesh(mesh.devices.reshape(4, 8, 4, 2), AXES)
    return jax.shard_map(
        shards,
        mesh=split,
        in_specs=(
            P(GX, GY, None, None, None),
            P(),
            P(),
            P(GX, GY, None),
            P(GX, GY, None),
            P(GX, GY, None, None),
            P(GX, GY, None),
        ),
        out_specs=(P(GX, GY, None, None, None), P(GX, GY, None, None, None)),
        check_vma=False,
    )
```

```python
import math

import jax
import jax.numpy as jnp
from jax import lax
from jax.experimental import pallas as pl
from jax.experimental.pallas import tpu as pltpu
from jax.sharding import Mesh
from jax.sharding import PartitionSpec as P

STEPS = 8
AXES = ("gx_0", "gx_1", "gy_0", "gy_1")
GX = ("gx_0", "gx_1")
GY = ("gy_0", "gy_1")

VMEM = pl.BlockSpec(memory_space=pltpu.VMEM)
SMEM = pl.BlockSpec(memory_space=pltpu.SMEM)
FAR = pl.BlockSpec(memory_space=pltpu.HBM)
PARAMS = pltpu.CompilerParams(vmem_limit_bytes=16 * 1024 * 1024)
F32 = jnp.float32


def tile_iota(axis):
    return lax.broadcasted_iota(jnp.int32, (8, 128), axis)


def shaped(*shape):
    return jax.ShapeDtypeStruct(shape, F32)


def prepare_kernel(class_scale, far_side, far_material, far_boundary, own, low, high, masked, *scratch):
    right_side, material, boundary, sems = scratch
    copies = [
        pltpu.make_async_copy(far_material, material, sems.at[0]),
        pltpu.make_async_copy(far_boundary, boundary, sems.at[1]),
        pltpu.make_async_copy(far_side, right_side, sems.at[2]),
    ]
    for copy in copies:
        copy.start()
    copies[0].wait()
    copies[1].wait()
    for x in range(2):
        for half in range(2):
            rows = pl.ds(half * 8, 8)
            field = jnp.zeros((8, 128), F32)
            kinds = material[x, rows]
            for number in range(8):
                field = field + jnp.where(kinds == number, class_scale[number], 0.0)
            field = jnp.where(boundary[x, rows] == 1, 0.0, field)
            masked[x, rows] = field
            (low, high)[x][pl.ds(384 + half * 8, 8)] = field

    copies[2].wait()

    def one_row(y, carry):
        for c in range(3):
            tile = jnp.concatenate([right_side[0, y, c], right_side[1, y, c]], axis=0)
            own[y, c] = tile
            low[pl.ds((y * 3 + c) * 8, 8)] = tile
            high[pl.ds((y * 3 + c) * 8, 8)] = tile
        return carry

    lax.fori_loop(0, 16, one_row, 0)


def prepare(class_scale, right_side, material, boundary):
    return pl.pallas_call(
        prepare_kernel,
        out_shape=(shaped(16, 3, 8, 128), shaped(400, 128), shaped(400, 128), shaped(2, 16, 128)),
        in_specs=[SMEM, FAR, FAR, FAR],
        out_specs=(VMEM,) * 4,
        scratch_shapes=[
            pltpu.VMEM((2, 16, 3, 4, 128), F32),
            pltpu.VMEM((2, 16, 128), jnp.int32),
            pltpu.VMEM((2, 16, 128), jnp.int32),
            pltpu.SemaphoreType.DMA((3,)),
        ],
        compiler_params=PARAMS,
        name="prepare",
    )(class_scale, right_side, material, boundary)


def setup_kernel(stencil, class_scale, rows, sign_bits, coef, interval, signs):
    def fill(n, total):
        tile = jnp.full((8, 128), stencil[n])
        coef[n] = tile
        return total + tile * tile

    total = lax.fori_loop(0, 243, fill, jnp.zeros((8, 128), F32))
    centre = [jnp.full((8, 128), stencil[13 * 9 + n]) for n in (0, 4, 8)]
    middle = (centre[0] + centre[1] + centre[2]) / 3.0
    for tile in centre:
        total = total - tile * tile
    spread = jnp.sqrt(jnp.maximum(total, 0.0) / 3.0)
    least = most = jnp.full((8, 128), class_scale[0])
    for number in range(1, 8):
        value = jnp.full((8, 128), class_scale[number])
        least, most = jnp.minimum(least, value), jnp.maximum(most, value)
    bottom = jnp.minimum(least * (middle - spread), 1.0)
    top = jnp.maximum(most * (middle + spread), 1.0)
    shift = 0.5 * (bottom + top)
    interval[0] = shift
    interval[1] = jnp.maximum(0.5 * (top - bottom), 0.05 * shift)

    lanes = lax.broadcasted_iota(jnp.int32, (1, 128), 1)
    size = 1.0 / math.sqrt(128.0)

    def sample(n, carry):
        for part in range(2):
            spot = rows[n + 64 * part]
            tile = lax.shift_right_logical(spot, 7)
            x = (tile >= 48).astype(jnp.int32)
            place = tile - 48 * x
            y = lax.shift_right_logical(place * 171, 9)
            bits = sign_bits[x, place - 3 * y, pl.ds(y, 1), :]
            common = (spot & 127) & lanes
            for by in (4, 2, 1):
                common = common ^ lax.shift_right_logical(common, by)
            row = jnp.where(((common ^ bits) & 1) == 1, size, -size)
            signs[n, pl.ds(4 * part, 4), :] = jnp.broadcast_to(row, (4, 128))
        return carry

    lax.fori_loop(0, 64, sample, 0, unroll=4)


def setup(stencil, class_scale, rows, sign_bits):
    return pl.pallas_call(
        setup_kernel,
        out_shape=(shaped(243, 8, 128), shaped(2, 8, 128), shaped(64, 8, 128)),
        in_specs=[SMEM, SMEM, SMEM, VMEM],
        out_specs=(VMEM,) * 3,
        compiler_params=PARAMS,
        name="setup",
    )(stencil, class_scale, rows, sign_bits)


def stencil_rows(coef, component, rows, terms):
    sums = [[None] * rows for _ in range(3)]
    for dx, tile in terms:
        for c in range(3):
            tiles = [tile(r, c) for r in range(rows + 2)]
            for dy in range(3):
                for dz in range(3):
                    weight = coef[(dx * 9 + dy * 3 + dz) * 9 + component * 3 + c]
                    for r in range(rows):
                        term = weight * tiles[r + dy]
                        old = sums[dz][r]
                        sums[dz][r] = term if old is None else old + term
    lane = tile_iota(1)
    out = []
    for r in range(rows):
        low = jnp.where(lane > 0, pltpu.roll(sums[0][r], 1, 1), 0.0)
        high = jnp.where(lane < 127, pltpu.roll(sums[2][r], 127, 1), 0.0)
        out.append(sums[1][r] + low + high)
    return out


def five_pairs(put, left, own, right):
    half = tile_iota(0) < 4
    turned = [pltpu.roll(tile, 4, 0) for tile in (left, own, right)]
    put(0, left)
    put(1, jnp.where(half, turned[0], turned[1]))
    put(2, own)
    put(3, jnp.where(half, turned[1], turned[2]))
    put(4, right)


def recurrence(interval):
    shift = interval[0]
    gain = 2.0 / interval[1]
    inside, fixed = -shift * gain, gain - shift * gain

    def value(alpha, total, centre):
        return (alpha * gain) * total + jnp.where(alpha == 0.0, fixed, inside) * centre

    return value


SEVEN = 7


def inner_kernel(coef, own, part):
    def body(i, carry):
        component, first, side = i % 3, i // 3 % 2 * SEVEN, i // 6
        terms = [(2 - 2 * side, lambda r, c: own[first + r, c])]
        for r, total in enumerate(stencil_rows(coef, component, SEVEN, terms)):
            part[first + r, side, component] = total
        return carry

    lax.fori_loop(0, 12, body, 0)


def inner(coef, own):
    return pl.pallas_call(
        inner_kernel,
        out_shape=shaped(14, 2, 3, 8, 128),
        in_specs=[VMEM, VMEM],
        out_specs=VMEM,
        compiler_params=PARAMS,
        name="inner",
    )(coef, own)


def make_middle_kernel(first_round):
    def kernel(coef, interval, left, own, right, part, before, scale, mid, work):
        def fill(y, carry):
            for c in range(3):

                def put(n, tile):
                    work[y, n, c] = tile

                five_pairs(put, left[y, c], own[y, c], right[y, c])
            return carry

        lax.fori_loop(0, 16, fill, 0)
        value_of = recurrence(interval)

        def body(i, carry):
            component, first, side = i % 3, i // 3 % 2 * SEVEN, i // 6
            terms = [
                (side + n, lambda r, c, n=n: work[first + r, 3 * side + n, c]) for n in range(2)
            ]
            for r, total in enumerate(stencil_rows(coef, component, SEVEN, terms)):
                row = first + r
                value = value_of(
                    scale[row + 1, side],
                    total + part[row, side, component],
                    work[row + 1, side * 2 + 1, component],
                )
                if first_round:
                    value = value * 0.5
                else:
                    value = value - before[row + 2, side * 2, component]
                mid[row + 2, side * 2, component] = value
            return carry

        lax.fori_loop(0, 12, body, 0)

    return kernel


def middle(first_round, *operands):
    return pl.pallas_call(
        make_middle_kernel(first_round),
        out_shape=shaped(18, 3, 3, 8, 128),
        in_specs=[VMEM] * 8,
        out_specs=VMEM,
        scratch_shapes=[pltpu.VMEM((16, 5, 3, 8, 128), F32)],
        compiler_params=PARAMS,
        name="middle",
    )(*operands)


def make_outer_kernel(first_round):
    def kernel(
        coef, interval, left, own, right, down, up, before, scale, scale_own, started, mid, last, work
    ):
        del started
        half = tile_iota(0) < 4
        value_of = recurrence(interval)
        for edge in range(2):
            for row in range(4):
                for c in range(3):

                    def put(n, tile):
                        work[edge, row, n, c] = tile

                    far = (down, up)[edge]
                    near = row - 2 + 14 * edge if edge == 0 else row + 14
                    if (row < 2) == (edge == 0):
                        five_pairs(put, *[far[n, row % 2, c] for n in range(3)])
                    else:
                        five_pairs(put, left[near, c], own[near, c], right[near, c])

        def edges(i, carry):
            component, edge = i % 3, i // 3
            for side in range(2):
                terms = [
                    (dx, lambda r, c, dx=dx: work[edge, r, side * 2 + dx, c]) for dx in range(3)
                ]
                for r, total in enumerate(stencil_rows(coef, component, 2, terms)):
                    row = edge * 16 + r
                    value = value_of(
                        scale[row, side], total, work[edge, r + 1, side * 2 + 1, component]
                    )
                    if first_round:
                        value = value * 0.5
                    else:
                        value = value - before[row, side * 2, component]
                    mid[row, side * 2, component] = value
            return carry

        lax.fori_loop(0, 6, edges, 0)

        def join(row, carry):
            for c in range(3):
                mid[row, 1, c] = jnp.where(
                    half, pltpu.roll(mid[row, 0, c], 4, 0), pltpu.roll(mid[row, 2, c], 4, 0)
                )
            return carry

        lax.fori_loop(0, 18, join, 0)

        def second(i, carry):
            component, first = i % 3, i // 3 * 8
            terms = [(dx, lambda r, c, dx=dx: mid[first + r, dx, c]) for dx in range(3)]
            for r, total in enumerate(stencil_rows(coef, component, 8, terms)):
                row = first + r
                value = value_of(scale_own[row], total, mid[row + 1, 1, component])
                last[row, component] = value - own[row, component]
            return carry

        lax.fori_loop(0, 6, second, 0)

    return kernel


def outer(first_round, *operands):
    return pl.pallas_call(
        make_outer_kernel(first_round),
        out_shape=(shaped(18, 3, 3, 8, 128), shaped(16, 3, 8, 128)),
        in_specs=[VMEM] * 11,
        out_specs=(VMEM, VMEM),
        scratch_shapes=[pltpu.VMEM((2, 4, 5, 3, 8, 128), F32)],
        input_output_aliases={10: 0},
        compiler_params=PARAMS,
        name="outer",
    )(*operands)


def make_sketch_kernel(kinds, earlier):
    def kernel(rows, signs, *refs):
        count = len(kinds)
        blocks, out, both = refs[:count], refs[-2], refs[-1]
        base = 0
        for part in refs[count : count + earlier]:
            size = part.shape[0]
            out[pl.ds(base, size), :] = part[...]
            base += size
        half = tile_iota(0) < 4
        lane = tile_iota(1)

        def spread(y, carry):
            for n, kind in enumerate(kinds):
                for c in range(3):
                    tile = blocks[n][y + 1, 1, c] if kind else blocks[n][y, c]
                    both[n, y * 3 + c] = tile
                    both[n, 48 + y * 3 + c] = pltpu.roll(tile, 4, 0)
            return carry

        lax.fori_loop(0, 16, spread, 0)

        def pick(group, sums):
            sums = list(sums)
            for k in range(8):
                j = group * 8 + k
                first = lax.shift_right_logical(rows[j], 7)
                second = lax.shift_right_logical(rows[64 + j], 7)
                second = jnp.where(second < 48, second + 48, second - 48)
                sign = signs[j]
                for n in range(count):
                    tile = jnp.where(half, both[n, first], both[n, second]) * sign
                    sums[n] = jnp.where(lane == j, jnp.sum(tile, axis=1, keepdims=True), sums[n])
            return tuple(sums)

        sums = lax.fori_loop(0, 8, pick, tuple(jnp.zeros((8, 128), F32) for _ in kinds))
        for n in range(count):
            folded = jnp.where(lane < 64, sums[n], pltpu.roll(pltpu.roll(sums[n], 64, 1), 4, 0))
            out[pl.ds(base + n * 4, 4), :] = folded[0:4]

    return kernel


def sketch(kinds, rows, signs, blocks, earlier=()):
    size = 4 * len(kinds) + sum(part.shape[0] for part in earlier)
    return pl.pallas_call(
        make_sketch_kernel(kinds, len(earlier)),
        out_shape=shaped(size, 128),
        in_specs=[SMEM] + [VMEM] * (1 + len(kinds) + len(earlier)),
        out_specs=VMEM,
        scratch_shapes=[pltpu.VMEM((len(kinds), 96, 8, 128), F32)],
        compiler_params=PARAMS,
        name="sketch",
    )(rows, signs, *blocks, *earlier)


def dot(a, b):
    return jnp.dot(a, b, precision=lax.Precision.HIGHEST, preferred_element_type=F32)


def sum_lanes(a):
    return jnp.sum(a, axis=1, keepdims=True)


def fit(table, shift, reach):
    lane = tile_iota(1)
    row = tile_iota(0)
    live = row < 4
    raise_by = jnp.where(lane < 4, reach, 0.5 * reach)
    lower_by = jnp.where(lane < 4, 0.0, 0.5 * reach)

    def move(coords):
        return (
            pltpu.roll(coords * raise_by, 4, 1)
            + shift * coords
            + pltpu.roll(coords * lower_by, 124, 1)
        )

    rhs = jnp.where(live, table[0:8], 0.0)
    norms = jnp.sqrt(sum_lanes(rhs * rhs) + 1e-06)
    basis = rhs / norms
    coords = jnp.where(live & (lane == row), 1.0, 0.0) / norms
    leading = jnp.sum(jnp.where(lane == row, coords, 0.0), axis=0, keepdims=True)
    for k in range(STEPS - 1):
        moved = move(coords)
        image = dot(moved[:, 0:40], table)
        rest, next_coords = image, moved
        for i in range(4):
            weight = sum_lanes(image * basis[i : i + 1])
            rest = rest - weight * basis[i : i + 1]
            next_coords = next_coords - weight * coords[i : i + 1]
        norms = jnp.sqrt(sum_lanes(rest * rest) + 1e-06)
        basis = rest / norms
        coords = next_coords / norms
        leading = leading + jnp.sum(
            jnp.where(live & (lane == row + 4 * (k + 1)), coords, 0.0), axis=0, keepdims=True
        )

    tall_row = lax.broadcasted_iota(jnp.int32, (40, 128), 0)
    tall_lane = lax.broadcasted_iota(jnp.int32, (40, 128), 1)
    wide = shift[0:1]
    part = 0.5 * reach[0:1]
    lower = jnp.concatenate([table[4:8], table[0:36]], axis=0)
    upper = jnp.concatenate([table[4:40], table[0:4]], axis=0)
    vectors = wide * table + part * (lower + upper)
    rhs_rows = jnp.concatenate([rhs, rhs, rhs, rhs, rhs], axis=0)
    vectors = jnp.where(tall_row < 32, vectors, rhs_rows)

    combos = jnp.where(tall_row == tall_lane, 1.0, 0.0)
    found = jnp.zeros((8, 128), F32)
    sizes = jnp.zeros((1, 128), F32)
    for j in range(4 * STEPS):
        pivot = vectors[j : j + 1]
        products = sum_lanes(vectors * pivot)
        size = products[j : j + 1]
        ratio = products / (size + 1e-37)
        found = jnp.where(lane == j, ratio[32:40], found)
        sizes = jnp.where(lane[0:1] == j, size, sizes)
        later = jnp.where(tall_row > j, ratio, 0.0)
        vectors = vectors - later * pivot
        combos = combos - later * combos[j : j + 1]
    scaled = sizes * leading * leading
    found = jnp.where(live, found * (scaled / (scaled + 1e-06)), 0.0)
    return move, dot(found[:, 0:40], combos)


def finish_kernel(table, interval, first, m0, l0, m1, l1, m2, l2, m3, l3, iterate, remainder, mix):
    shift, reach = interval[0], interval[1]
    lane = tile_iota(1)
    row = tile_iota(0)
    sub = row % 4
    total = table[0]
    for n in range(1, table.shape[0]):
        total = total + table[n]
    tall = jnp.concatenate([total, jnp.zeros((4, 128), F32)], axis=0)
    move, weights = fit(tall, shift, reach)
    weights = jnp.where(lane < 4 * STEPS, weights, 0.0)
    images = move(weights)
    weights = jnp.where(row < 4, weights, pltpu.roll(weights, 4, 0))
    images = jnp.where(row < 4, images, pltpu.roll(images, 4, 0))
    for k in range(STEPS + 1):
        for r in range(4):
            spot = lane == 4 * k + (sub + r) % 4
            if k < STEPS:
                mix[0, k * 4 + r] = jnp.broadcast_to(
                    sum_lanes(jnp.where(spot, weights, 0.0)), (8, 128)
                )
            mix[1, k * 4 + r] = jnp.broadcast_to(
                sum_lanes(jnp.where(spot, images, 0.0)), (8, 128)
            )

    refs = [(first, 0), (m0, 1), (l0, 0), (m1, 1), (l1, 0), (m2, 1), (l2, 0), (m3, 1), (l3, 0)]

    def one_row(y, carry):
        for c in range(3):
            total = None
            image = first[y, c]
            for k, (ref, kind) in enumerate(refs):
                tile = ref[y + 1, 1, c] if kind else ref[y, c]
                for r in range(4):
                    if r:
                        turned = jnp.where(
                            sub < 4 - r, pltpu.roll(tile, 8 - r, 0), pltpu.roll(tile, 4 - r, 0)
                        )
                    else:
                        turned = tile
                    if k < STEPS:
                        part = mix[0, k * 4 + r] * turned
                        total = part if total is None else total + part
                    image = image - mix[1, k * 4 + r] * turned
            for x in range(2):
                iterate[x, y, c] = total[4 * x : 4 * x + 4]
                remainder[x, y, c] = image[4 * x : 4 * x + 4]
        return carry

    lax.fori_loop(0, 16, one_row, 0)


def finish(table, interval, blocks):
    return pl.pallas_call(
        finish_kernel,
        out_shape=(shaped(2, 16, 3, 4, 128), shaped(2, 16, 3, 4, 128)),
        in_specs=[VMEM] * 11,
        out_specs=(VMEM, VMEM),
        scratch_shapes=[pltpu.VMEM((2, 36, 8, 128), F32)],
        compiler_params=PARAMS,
        name="finish",
    )(table, interval, *blocks)


def neighbours(low, high, axis):
    count = lax.axis_size(axis)
    after = lax.ppermute(low, axis, [(i + 1, i) for i in range(count - 1)])
    before = lax.ppermute(high, axis, [(i, i + 1) for i in range(count - 1)])
    return before, after


def fold(copies, count):
    def kernel(parts, out):
        total = parts[0]
        for n in range(1, copies.shape[0]):
            total = total + parts[n]
        for n in range(count):
            out[n] = total

    return pl.pallas_call(
        kernel,
        out_shape=shaped(count, *copies.shape[1:]),
        in_specs=[VMEM],
        out_specs=VMEM,
        compiler_params=PARAMS,
        name="fold",
    )(copies)


def cycle(right_side, stencil, class_scale, material, boundary, sign_bits, sample_rows):
    rows = sample_rows.reshape(-1)
    own, low, high, masked = prepare(
        class_scale, right_side.transpose(0, 1, 3, 2, 4), material, boundary
    )
    blocks = [own]
    sketches = []

    def spread(planes, count):
        pairs = planes.reshape(2, 2, count, 128).transpose(2, 0, 1, 3)
        return jnp.broadcast_to(pairs[:, :, :, None], (count, 2, 2, 4, 128)).reshape(
            count, 2, 8, 128
        )

    for turn in range(STEPS // 2):
        first_round = turn == 0
        if first_round:
            low, high = neighbours(low, high, GX)
            coef, interval, signs = setup(
                stencil.reshape(-1), class_scale, rows, sign_bits.transpose(0, 2, 1, 3)
            )
        else:
            left, right = neighbours(own, own, GX)
        part = sketch((0,) if first_round else (1, 0), rows, signs, blocks[-2:])
        started = inner(coef, own)
        if first_round:
            low, high, part, started, masked = lax.optimization_barrier(
                (low, high, part, started, masked)
            )
            left, right = low[:384].reshape(own.shape), high[:384].reshape(own.shape)
            planes = jnp.concatenate([low[None, 384:], masked, high[None, 384:]])
        else:
            left, right, part, started = lax.optimization_barrier((left, right, part, started))
        sketches.append(part)
        bottom = jnp.stack([left[:2], own[:2], right[:2]])
        top = jnp.stack([left[14:], own[14:], right[14:]])
        if first_round:
            flat_y = (3 * 2 * 3 * 8, 128)
            down, up = neighbours(
                jnp.concatenate([bottom.reshape(flat_y), planes[:, 0], planes[:, 0]]),
                jnp.concatenate([top.reshape(flat_y), planes[:, 15], planes[:, 15]]),
                GY,
            )
            scale_mid = spread(planes, 16)
            scale_own = jnp.broadcast_to(
                masked.transpose(1, 0, 2)[:, :, None], (16, 2, 4, 128)
            ).reshape(16, 8, 128)
            before = interval
        else:
            down, up = neighbours(bottom, top, GY)
            before = blocks[-2]
        started = middle(first_round, coef, interval, left, own, right, started, before, scale_mid)
        if first_round:
            down, up, started, scale_own = lax.optimization_barrier((down, up, started, scale_own))
            planes = jnp.concatenate([down[144:148, None], planes, up[144:148, None]], axis=1)
            down, up = down[:144].reshape(bottom.shape), up[:144].reshape(top.shape)
            scale = spread(planes, 18)
        mid, own = outer(
            first_round,
            *(coef, interval, left, own, right, down, up, before, scale, scale_own, started),
        )
        blocks += [mid, own]

    table = lax.psum(sketch((1, 0), rows, signs, blocks[-2:], sketches), "gy_1")
    copies = jnp.broadcast_to(table, (16,) + table.shape)
    copies = lax.all_to_all(copies, ("gx_0", "gy_0"), 0, 0, tiled=True)
    copies = lax.all_to_all(fold(copies, 8), ("gx_1",), 0, 0, tiled=True)
    iterate, remainder = finish(copies, interval, blocks)
    return iterate.transpose(0, 1, 3, 2, 4), remainder.transpose(0, 1, 3, 2, 4)


def solution(mesh):
    split = Mesh(mesh.devices.reshape(4, 8, 4, 2), AXES)
    return jax.shard_map(
        cycle,
        mesh=split,
        in_specs=(
            P(GX, GY, None, None, None),
            P(),
            P(),
            P(GX, GY, None),
            P(GX, GY, None),
            P(GX, GY, None, None),
            P(GX, GY, None),
        ),
        out_specs=(P(GX, GY, None, None, None), P(GX, GY, None, None, None)),
        check_vma=False,
    )
```

```python
import math

import jax
import jax.numpy as jnp
from jax import lax
from jax.experimental import pallas as pl
from jax.experimental.pallas import tpu as pltpu
from jax.sharding import Mesh
from jax.sharding import PartitionSpec as P

STEPS = 8
AXES = ("gx_0", "gx_1", "gy_0", "gy_1")
GX = ("gx_0", "gx_1")
GY = ("gy_0", "gy_1")

VMEM = pl.BlockSpec(memory_space=pltpu.VMEM)
SMEM = pl.BlockSpec(memory_space=pltpu.SMEM)
FAR = pl.BlockSpec(memory_space=pltpu.HBM)
PARAMS = pltpu.CompilerParams(vmem_limit_bytes=16 * 1024 * 1024)
F32 = jnp.float32


def tile_iota(axis):
    return lax.broadcasted_iota(jnp.int32, (8, 128), axis)


def shaped(*shape):
    return jax.ShapeDtypeStruct(shape, F32)


def prepare_kernel(class_scale, parity, far_side, far_material, far_boundary, own, first, second, masked, *scratch):
    right_side, material, boundary, sems = scratch
    copies = [
        pltpu.make_async_copy(far_material, material, sems.at[0]),
        pltpu.make_async_copy(far_boundary, boundary, sems.at[1]),
        pltpu.make_async_copy(far_side, right_side, sems.at[2]),
    ]
    for copy in copies:
        copy.start()
    copies[0].wait()
    copies[1].wait()
    even = parity[0] != 0.0
    for half in range(2):
        rows = pl.ds(half * 8, 8)
        fields = []
        for x in range(2):
            field = jnp.zeros((8, 128), F32)
            kinds = material[x, rows]
            for number in range(8):
                field = field + jnp.where(kinds == number, class_scale[number], 0.0)
            field = jnp.where(boundary[x, rows] == 1, 0.0, field)
            masked[x, rows] = field
            fields.append(field)
        first[pl.ds(384 + half * 8, 8)] = jnp.where(even, fields[1], fields[0])
        second[pl.ds(384 + half * 8, 8)] = jnp.where(even, fields[0], fields[1])

    copies[2].wait()

    def one_row(y, carry):
        for c in range(3):
            tile = jnp.concatenate([right_side[0, y, c], right_side[1, y, c]], axis=0)
            own[y, c] = tile
            first[pl.ds((y * 3 + c) * 8, 8)] = tile
            second[pl.ds((y * 3 + c) * 8, 8)] = tile
        return carry

    lax.fori_loop(0, 16, one_row, 0)


def prepare(class_scale, parity, *operands):
    return pl.pallas_call(
        prepare_kernel,
        out_shape=(shaped(16, 3, 8, 128), shaped(400, 128), shaped(400, 128), shaped(2, 16, 128)),
        in_specs=[SMEM, VMEM, FAR, FAR, FAR],
        out_specs=(VMEM,) * 4,
        scratch_shapes=[
            pltpu.VMEM((2, 16, 3, 4, 128), F32),
            pltpu.VMEM((2, 16, 128), jnp.int32),
            pltpu.VMEM((2, 16, 128), jnp.int32),
            pltpu.SemaphoreType.DMA((3,)),
        ],
        compiler_params=PARAMS,
        name="prepare",
    )(class_scale, parity, *[pltpu.with_memory_space_constraint(x, pltpu.HBM) for x in operands])


def setup_kernel(stencil, class_scale, coef, interval):
    def fill(n, total):
        for k in range(9):
            tile = jnp.full((8, 128), stencil[n * 9 + k])
            coef[n * 9 + k] = tile
            total = total + tile * tile
        return total

    total = lax.fori_loop(0, 27, fill, jnp.zeros((8, 128), F32))
    centre = [jnp.full((8, 128), stencil[13 * 9 + n]) for n in (0, 4, 8)]
    middle = (centre[0] + centre[1] + centre[2]) / 3.0
    for tile in centre:
        total = total - tile * tile
    spread = jnp.sqrt(jnp.maximum(total, 0.0) / 3.0)
    least = most = jnp.full((8, 128), class_scale[0])
    for number in range(1, 8):
        value = jnp.full((8, 128), class_scale[number])
        least, most = jnp.minimum(least, value), jnp.maximum(most, value)
    bottom = jnp.minimum(least * (middle - spread), 1.0)
    top = jnp.maximum(most * (middle + spread), 1.0)
    shift = 0.5 * (bottom + top)
    interval[0] = shift
    interval[1] = jnp.maximum(0.5 * (top - bottom), 0.05 * shift)


def setup(stencil, class_scale):
    return pl.pallas_call(
        setup_kernel,
        out_shape=(shaped(243, 8, 128), shaped(2, 8, 128)),
        in_specs=[SMEM, SMEM],
        out_specs=(VMEM,) * 2,
        compiler_params=PARAMS,
        name="setup",
    )(stencil, class_scale)


def signs_kernel(rows, sign_bits, signs):
    lanes = lax.broadcasted_iota(jnp.int32, (1, 128), 1)
    size = 1.0 / math.sqrt(128.0)

    def sample(n, carry):
        for part in range(2):
            spot = rows[n + 64 * part]
            tile = lax.shift_right_logical(spot, 7)
            x = (tile >= 48).astype(jnp.int32)
            place = tile - 48 * x
            y = lax.shift_right_logical(place * 171, 9)
            bits = sign_bits[x, place - 3 * y, pl.ds(y, 1), :]
            common = (spot & 127) & lanes
            for by in (4, 2, 1):
                common = common ^ lax.shift_right_logical(common, by)
            row = jnp.where(((common ^ bits) & 1) == 1, size, -size)
            signs[n, pl.ds(4 * part, 4), :] = jnp.broadcast_to(row, (4, 128))
        return carry

    lax.fori_loop(0, 64, sample, 0, unroll=8)


def sample_signs(rows, sign_bits):
    return pl.pallas_call(
        signs_kernel,
        out_shape=shaped(64, 8, 128),
        in_specs=[SMEM, VMEM],
        out_specs=VMEM,
        compiler_params=PARAMS,
        name="signs",
    )(rows, sign_bits)


def stencil_rows(coef, component, rows, terms):
    sums = [[None] * rows for _ in range(3)]
    for dx, tile in terms:
        for c in range(3):
            tiles = [tile(r, c) for r in range(rows + 2)]
            for dy in range(3):
                for dz in range(3):
                    weight = coef[(dx * 9 + dy * 3 + dz) * 9 + component * 3 + c]
                    for r in range(rows):
                        term = weight * tiles[r + dy]
                        old = sums[dz][r]
                        sums[dz][r] = term if old is None else old + term
    lane = tile_iota(1)
    out = []
    for r in range(rows):
        low = jnp.where(lane > 0, pltpu.roll(sums[0][r], 1, 1), 0.0)
        high = jnp.where(lane < 127, pltpu.roll(sums[2][r], 127, 1), 0.0)
        out.append(sums[1][r] + low + high)
    return out


def five_pairs(put, left, own, right):
    half = tile_iota(0) < 4
    turned = [pltpu.roll(tile, 4, 0) for tile in (left, own, right)]
    put(0, left)
    put(1, jnp.where(half, turned[0], turned[1]))
    put(2, own)
    put(3, jnp.where(half, turned[1], turned[2]))
    put(4, right)


def recurrence(interval):
    shift = interval[0]
    gain = 2.0 / interval[1]
    inside, fixed = -shift * gain, gain - shift * gain

    def value(alpha, total, centre):
        return (alpha * gain) * total + jnp.where(alpha == 0.0, fixed, inside) * centre

    return value


SEVEN = 7


def inner_kernel(coef, own, part, turned):
    def turn_rows(y, carry):
        for c in range(3):
            turned[y, c] = pltpu.roll(own[y, c], 4, 0)
        return carry

    lax.fori_loop(0, 16, turn_rows, 0)

    def body(i, carry):
        component, first = i % 3, i // 3 * SEVEN
        for n, (dx, source) in enumerate(((2, own), (1, turned), (0, own))):
            terms = [(dx, lambda r, c, source=source: source[first + r, c])]
            for r, total in enumerate(stencil_rows(coef, component, SEVEN, terms)):
                part[first + r, n, component] = total
        return carry

    lax.fori_loop(0, 6, body, 0)


def inner(coef, own):
    return pl.pallas_call(
        inner_kernel,
        out_shape=shaped(14, 3, 3, 8, 128),
        in_specs=[VMEM, VMEM],
        out_specs=VMEM,
        scratch_shapes=[pltpu.VMEM((16, 3, 8, 128), F32)],
        compiler_params=PARAMS,
        name="inner",
    )(coef, own)


def second_step(mid, own, scale_own, value_of, coef, component, first, rows, last):
    terms = [(dx, lambda r, c, dx=dx: mid[first + r, dx, c]) for dx in range(3)]
    for r, total in enumerate(stencil_rows(coef, component, rows, terms)):
        row = first + r
        value = value_of(scale_own[row], total, mid[row + 1, 1, component])
        last[row, component] = value - own[row, component]


def join(mid, row):
    half = tile_iota(0) < 4
    for c in range(3):
        mid[row, 1, c] = jnp.where(
            half, pltpu.roll(mid[row, 0, c], 4, 0), pltpu.roll(mid[row, 2, c], 4, 0)
        )


def make_middle_kernel(first_round):
    def kernel(
        coef, interval, parity, swap_a, own, swap_b, part, before, scale, scale_own, mid, last,
        left, right, beside,
    ):
        half = tile_iota(0) < 4
        even = parity[0] != 0.0

        def fill(y, carry):
            for c in range(3):
                a, b = swap_a[y, c], swap_b[y, c]
                lower, upper = jnp.where(even, b, a), jnp.where(even, a, b)
                left[y, c] = lower
                right[y, c] = upper
                beside[y, c] = pltpu.roll(jnp.where(half, upper, lower), 4, 0)
            return carry

        lax.fori_loop(0, 16, fill, 0)
        value_of = recurrence(interval)

        def body(i, carry):
            component, first = i % 3, i // 3 * SEVEN
            sums = []
            for dx, source in ((0, left), (1, beside), (2, right)):
                terms = [(dx, lambda r, c, source=source: source[first + r, c])]
                sums.append(stencil_rows(coef, component, SEVEN, terms))
            for r in range(SEVEN):
                row = first + r
                near, far = part[row, 1, component], sums[1][r]
                turned = pltpu.roll(own[row + 1, component], 4, 0)
                centre = beside[row + 1, component]
                for side in range(2):
                    pick = half if side == 0 else jnp.logical_not(half)
                    total = sums[2 * side][r] + part[row, 2 * side, component]
                    value = value_of(
                        scale[row + 1, side],
                        total + jnp.where(pick, far, near),
                        jnp.where(pick, centre, turned),
                    )
                    if first_round:
                        value = value * 0.5
                    else:
                        value = value - before[row + 2, side * 2, component]
                    mid[row + 2, side * 2, component] = value
            return carry

        lax.fori_loop(0, 6, body, 0)

        def join_rows(row, carry):
            join(mid, row + 2)
            return carry

        lax.fori_loop(0, 14, join_rows, 0)

        def second(i, carry):
            second_step(mid, own, scale_own, value_of, coef, i % 3, 2 + i // 3 * 6, 6, last)
            return carry

        lax.fori_loop(0, 6, second, 0)

    return kernel


def middle(first_round, *operands):
    return pl.pallas_call(
        make_middle_kernel(first_round),
        out_shape=(shaped(18, 3, 3, 8, 128), shaped(16, 3, 8, 128)),
        in_specs=[VMEM] * 10,
        out_specs=(VMEM, VMEM),
        scratch_shapes=[pltpu.VMEM((16, 3, 8, 128), F32)] * 3,
        compiler_params=PARAMS,
        name="middle",
    )(*operands)


def make_outer_kernel(first_round):
    def kernel(
        coef, interval, parity, swap_a, own, swap_b, swap_c, swap_d, before, scale, scale_own,
        scale_far, mid_before, last_before, mid, last, *rest,
    ):
        del mid_before, last_before
        work = rest[-1]
        value_of = recurrence(interval)
        even_x, even_y = parity[0] != 0.0, parity[1] != 0.0
        edge_scale = rest[-2]

        def message(n, row, c):
            if not first_round:
                return swap_c[n, row, c], swap_d[n, row, c]
            spot = pl.ds(((n * 2 + row) * 3 + c) * 8, 8)
            return swap_c[spot], swap_d[spot]

        for edge in range(2):
            for row in range(4):
                for c in range(3):

                    def put(n, tile):
                        work[edge, row, n, c] = tile

                    if (row < 2) == (edge == 0):
                        tiles = []
                        for n in range(3):
                            a, b = message(n, row % 2, c)
                            tiles.append(jnp.where(even_y, a, b) if edge else jnp.where(even_y, b, a))
                        five_pairs(put, *tiles)
                    else:
                        near = row - 2 if edge == 0 else row + 14
                        a, b = swap_a[near, c], swap_b[near, c]
                        five_pairs(
                            put, jnp.where(even_x, b, a), own[near, c], jnp.where(even_x, a, b)
                        )
            for side in range(2):
                if first_round:
                    planes = []
                    for x in range(2):
                        spot = pl.ds(144 + 2 * side + x, 1)
                        a, b = swap_c[spot], swap_d[spot]
                        row = jnp.where(even_y[0:1], a, b) if edge else jnp.where(even_y[0:1], b, a)
                        planes.append(jnp.broadcast_to(row, (8, 128)))
                    far_tile = jnp.where(tile_iota(0) < 4, planes[0], planes[1])
                    rest[0][edge, side] = far_tile
                else:
                    far_tile = scale_far[edge, side]
                edge_scale[edge, edge, side] = far_tile
                edge_scale[edge, 1 - edge, side] = scale[15 * edge, side]

        def edges(i, carry):
            component, edge = i % 3, i // 3
            for side in range(2):
                terms = [
                    (dx, lambda r, c, dx=dx: work[edge, r, side * 2 + dx, c]) for dx in range(3)
                ]
                for r, total in enumerate(stencil_rows(coef, component, 2, terms)):
                    row = edge * 16 + r
                    value = value_of(
                        edge_scale[edge, r, side], total, work[edge, r + 1, side * 2 + 1, component]
                    )
                    if first_round:
                        value = value * 0.5
                    else:
                        value = value - before[row, side * 2, component]
                    mid[row, side * 2, component] = value
            return carry

        lax.fori_loop(0, 6, edges, 0)
        for row in (0, 1, 16, 17):
            join(mid, row)

        def second(i, carry):
            second_step(mid, own, scale_own, value_of, coef, i % 3, i // 3 * 14, 2, last)
            return carry

        lax.fori_loop(0, 6, second, 0)

    return kernel


def outer(first_round, *operands):
    far = (shaped(2, 2, 8, 128),) if first_round else ()
    return pl.pallas_call(
        make_outer_kernel(first_round),
        out_shape=(shaped(18, 3, 3, 8, 128), shaped(16, 3, 8, 128), *far),
        in_specs=[VMEM] * 14,
        out_specs=(VMEM,) * (2 + len(far)),
        scratch_shapes=[
            pltpu.VMEM((2, 2, 2, 8, 128), F32),
            pltpu.VMEM((2, 4, 5, 3, 8, 128), F32),
        ],
        input_output_aliases={12: 0, 13: 1},
        compiler_params=PARAMS,
        name="outer",
    )(*operands)


def make_sketch_kernel(kinds, earlier):
    def kernel(rows, signs, *refs):
        count = len(kinds)
        blocks, out, both = refs[:count], refs[-2], refs[-1]
        base = 0
        for part in refs[count : count + earlier]:
            size = part.shape[0]
            out[pl.ds(base, size), :] = part[...]
            base += size
        half = tile_iota(0) < 4
        lane = tile_iota(1)

        def spread(y, carry):
            for n, kind in enumerate(kinds):
                for c in range(3):
                    tile = blocks[n][y + 1, 1, c] if kind else blocks[n][y, c]
                    both[n, y * 3 + c] = tile
                    both[n, 48 + y * 3 + c] = pltpu.roll(tile, 4, 0)
            return carry

        lax.fori_loop(0, 16, spread, 0)

        sums = [jnp.zeros((8, 128), F32)] * count
        for j in range(64):
            first = lax.shift_right_logical(rows[j], 7)
            second = lax.shift_right_logical(rows[64 + j], 7)
            second = jnp.where(second < 48, second + 48, second - 48)
            sign = signs[j]
            for n in range(count):
                tile = jnp.where(half, both[n, first], both[n, second]) * sign
                sums[n] = jnp.where(lane == j, jnp.sum(tile, axis=1, keepdims=True), sums[n])
        for n in range(count):
            folded = jnp.where(lane < 64, sums[n], pltpu.roll(pltpu.roll(sums[n], 64, 1), 4, 0))
            out[pl.ds(base + n * 4, 4), :] = folded[0:4]

    return kernel


def sketch(kinds, rows, signs, blocks, earlier=()):
    size = 4 * len(kinds) + sum(part.shape[0] for part in earlier)
    return pl.pallas_call(
        make_sketch_kernel(kinds, len(earlier)),
        out_shape=shaped(size, 128),
        in_specs=[SMEM] + [VMEM] * (1 + len(kinds) + len(earlier)),
        out_specs=VMEM,
        scratch_shapes=[pltpu.VMEM((len(kinds), 96, 8, 128), F32)],
        compiler_params=PARAMS,
        name="sketch",
    )(rows, signs, *blocks, *earlier)


def dot(a, b):
    return jnp.dot(a, b, precision=lax.Precision.HIGHEST, preferred_element_type=F32)


def sum_lanes(a):
    return jnp.sum(a, axis=1, keepdims=True)


def fit(table, shift, reach):
    lane = tile_iota(1)
    row = tile_iota(0)
    live = row < 4
    raise_by = jnp.where(lane < 4, reach, 0.5 * reach)
    lower_by = jnp.where(lane < 4, 0.0, 0.5 * reach)

    def move(coords):
        return (
            pltpu.roll(coords * raise_by, 4, 1)
            + shift * coords
            + pltpu.roll(coords * lower_by, 124, 1)
        )

    rhs = jnp.where(live, table[0:8], 0.0)
    norms = jnp.sqrt(sum_lanes(rhs * rhs) + 1e-06)
    basis = rhs / norms
    coords = jnp.where(live & (lane == row), 1.0, 0.0) / norms
    leading = jnp.sum(jnp.where(lane == row, coords, 0.0), axis=0, keepdims=True)
    for k in range(STEPS - 1):
        moved = move(coords)
        image = dot(moved[:, 0:40], table)
        rest, next_coords = image, moved
        for i in range(4):
            weight = sum_lanes(image * basis[i : i + 1])
            rest = rest - weight * basis[i : i + 1]
            next_coords = next_coords - weight * coords[i : i + 1]
        norms = jnp.sqrt(sum_lanes(rest * rest) + 1e-06)
        basis = rest / norms
        coords = next_coords / norms
        leading = leading + jnp.sum(
            jnp.where(live & (lane == row + 4 * (k + 1)), coords, 0.0), axis=0, keepdims=True
        )

    tall_row = lax.broadcasted_iota(jnp.int32, (40, 128), 0)
    tall_lane = lax.broadcasted_iota(jnp.int32, (40, 128), 1)
    wide = shift[0:1]
    part = 0.5 * reach[0:1]
    lower = jnp.concatenate([table[4:8], table[0:36]], axis=0)
    upper = jnp.concatenate([table[4:40], table[0:4]], axis=0)
    vectors = wide * table + part * (lower + upper)
    rhs_rows = jnp.concatenate([rhs, rhs, rhs, rhs, rhs], axis=0)
    vectors = jnp.where(tall_row < 32, vectors, rhs_rows)

    combos = jnp.where(tall_row == tall_lane, 1.0, 0.0)
    found = jnp.zeros((8, 128), F32)
    sizes = jnp.zeros((1, 128), F32)
    for j in range(4 * STEPS):
        pivot = vectors[j : j + 1]
        products = sum_lanes(vectors * pivot)
        size = products[j : j + 1]
        ratio = products / (size + 1e-37)
        found = jnp.where(lane == j, ratio[32:40], found)
        sizes = jnp.where(lane[0:1] == j, size, sizes)
        later = jnp.where(tall_row > j, ratio, 0.0)
        vectors = vectors - later * pivot
        combos = combos - later * combos[j : j + 1]
    scaled = sizes * leading * leading
    found = jnp.where(live, found * (scaled / (scaled + 1e-06)), 0.0)
    return move, dot(found[:, 0:40], combos)


def finish_kernel(table, interval, first, m0, l0, m1, l1, m2, l2, m3, l3, iterate, remainder, mix):
    shift, reach = interval[0], interval[1]
    lane = tile_iota(1)
    row = tile_iota(0)
    sub = row % 4
    total = table[0]
    for n in range(1, table.shape[0]):
        total = total + table[n]
    tall = jnp.concatenate([total, jnp.zeros((4, 128), F32)], axis=0)
    move, weights = fit(tall, shift, reach)
    weights = jnp.where(lane < 4 * STEPS, weights, 0.0)
    images = move(weights)
    weights = jnp.where(row < 4, weights, pltpu.roll(weights, 4, 0))
    images = jnp.where(row < 4, images, pltpu.roll(images, 4, 0))
    for k in range(STEPS + 1):
        for r in range(4):
            spot = lane == 4 * k + (sub + r) % 4
            if k < STEPS:
                mix[0, k * 4 + r] = jnp.broadcast_to(
                    sum_lanes(jnp.where(spot, weights, 0.0)), (8, 128)
                )
            mix[1, k * 4 + r] = jnp.broadcast_to(
                sum_lanes(jnp.where(spot, images, 0.0)), (8, 128)
            )

    refs = [(first, 0), (m0, 1), (l0, 0), (m1, 1), (l1, 0), (m2, 1), (l2, 0), (m3, 1), (l3, 0)]

    def one_row(y, carry):
        for c in range(3):
            total = None
            image = first[y, c]
            for k, (ref, kind) in enumerate(refs):
                tile = ref[y + 1, 1, c] if kind else ref[y, c]
                for r in range(4):
                    if r:
                        turned = jnp.where(
                            sub < 4 - r, pltpu.roll(tile, 8 - r, 0), pltpu.roll(tile, 4 - r, 0)
                        )
                    else:
                        turned = tile
                    if k < STEPS:
                        part = mix[0, k * 4 + r] * turned
                        total = part if total is None else total + part
                    image = image - mix[1, k * 4 + r] * turned
            for x in range(2):
                iterate[x, y, c] = total[4 * x : 4 * x + 4]
                remainder[x, y, c] = image[4 * x : 4 * x + 4]
        return carry

    lax.fori_loop(0, 16, one_row, 0)


def finish(table, interval, blocks):
    return pl.pallas_call(
        finish_kernel,
        out_shape=(shaped(2, 16, 3, 4, 128), shaped(2, 16, 3, 4, 128)),
        in_specs=[VMEM] * 11,
        out_specs=(VMEM, VMEM),
        scratch_shapes=[pltpu.VMEM((2, 36, 8, 128), F32)],
        compiler_params=PARAMS,
        name="finish",
    )(table, interval, *blocks)


def swap(first, second, axis):
    count = lax.axis_size(axis)
    out = []
    for start, operand in ((0, first), (1, second)):
        pairs = [(i + k, i + 1 - k) for i in range(start, count - 1, 2) for k in range(2)]
        out.append(lax.ppermute(operand, axis, pairs))
    return out


def fold(copies, count):
    def kernel(parts, out):
        total = parts[0]
        for n in range(1, copies.shape[0]):
            total = total + parts[n]
        for n in range(count):
            out[n] = total

    return pl.pallas_call(
        kernel,
        out_shape=shaped(count, *copies.shape[1:]),
        in_specs=[VMEM],
        out_specs=VMEM,
        compiler_params=PARAMS,
        name="fold",
    )(copies)


def cycle(right_side, stencil, class_scale, material, boundary, sign_bits, sample_rows):
    rows = sample_rows.reshape(-1)
    flags = [lax.axis_index(axis) % 2 == 0 for axis in (GX, GY)]
    parity = jnp.stack([jnp.broadcast_to(flag.astype(F32), (8, 128)) for flag in flags])
    own, first, second, masked = prepare(
        class_scale, parity, right_side.transpose(0, 1, 3, 2, 4), material, boundary
    )
    blocks = [own]
    sketches = []

    for turn in range(STEPS // 2):
        first_round = turn == 0
        if first_round:
            swap_a, swap_b = swap(first, second, GX)
            coef, interval = setup(stencil.reshape(-1), class_scale)
        else:
            swap_a, swap_b = swap(own, own, GX)
        if turn == 1:
            signs = sample_signs(rows, sign_bits.transpose(0, 2, 1, 3))
        if not first_round:
            kinds = (0, 1, 0) if turn == 1 else (1, 0)
            part = sketch(kinds, rows, signs, blocks[-len(kinds) :])
        started = inner(coef, own)
        if first_round:
            swap_a, swap_b, started, masked = lax.optimization_barrier(
                (swap_a, swap_b, started, masked)
            )
            planes = [swap_a[None, 384:], swap_b[None, 384:]]
            planes = jnp.concatenate(
                [
                    jnp.where(flags[0], planes[1], planes[0]),
                    masked,
                    jnp.where(flags[0], planes[0], planes[1]),
                ]
            )
            swap_a, swap_b = swap_a[:384].reshape(own.shape), swap_b[:384].reshape(own.shape)
        else:
            swap_a, swap_b, part, started = lax.optimization_barrier(
                (swap_a, swap_b, part, started)
            )
            sketches.append(part)

        def ends(first):
            a, b = swap_a[first : first + 2], swap_b[first : first + 2]
            return jnp.stack(
                [
                    jnp.where(flags[0], b, a),
                    own[first : first + 2],
                    jnp.where(flags[0], a, b),
                ]
            )

        bottom, top = ends(0), ends(14)
        if first_round:
            flat = (3 * 2 * 3 * 8, 128)
            bottom = jnp.concatenate([bottom.reshape(flat), planes[:, 0], planes[:, 0]])
            top = jnp.concatenate([top.reshape(flat), planes[:, 15], planes[:, 15]])
        swap_c, swap_d = swap(
            jnp.where(flags[1], top, bottom), jnp.where(flags[1], bottom, top), GY
        )
        if first_round:
            pairs = planes.reshape(2, 2, 16, 128).transpose(2, 0, 1, 3)
            scale = jnp.broadcast_to(pairs[:, :, :, None], (16, 2, 2, 4, 128))
            scale = scale.reshape(16, 2, 8, 128)
            scale_own = jnp.broadcast_to(
                masked.transpose(1, 0, 2)[:, :, None], (16, 2, 4, 128)
            ).reshape(16, 8, 128)
            before = scale_far = interval
        else:
            before = blocks[-2]
        shared = (coef, interval, parity, swap_a, own, swap_b)
        started = middle(first_round, *shared, started, before, scale, scale_own)
        done = outer(
            first_round,
            *shared,
            *(swap_c, swap_d, before, scale, scale_own, scale_far, *started),
        )
        if first_round:
            scale_far = done[2]
        own = done[1]
        blocks += done[:2]

    table = lax.psum(sketch((1, 0), rows, signs, blocks[-2:], sketches), "gy_1")
    copies = jnp.broadcast_to(table, (16,) + table.shape)
    copies = lax.all_to_all(copies, ("gx_0", "gy_0"), 0, 0, tiled=True)
    copies = lax.all_to_all(fold(copies, 8), ("gx_1",), 0, 0, tiled=True)
    iterate, remainder = finish(copies, interval, blocks)
    return iterate.transpose(0, 1, 3, 2, 4), remainder.transpose(0, 1, 3, 2, 4)


def solution(mesh):
    split = Mesh(mesh.devices.reshape(4, 8, 4, 2), AXES)
    return jax.shard_map(
        cycle,
        mesh=split,
        in_specs=(
            P(GX, GY, None, None, None),
            P(),
            P(),
            P(GX, GY, None),
            P(GX, GY, None),
            P(GX, GY, None, None),
            P(GX, GY, None),
        ),
        out_specs=(P(GX, GY, None, None, None), P(GX, GY, None, None, None)),
        check_vma=False,
    )
```

```python
import math

import jax
import jax.numpy as jnp
from jax import lax
from jax.experimental import pallas as pl
from jax.experimental.pallas import tpu as pltpu
from jax.sharding import Mesh
from jax.sharding import PartitionSpec as P

STEPS = 8
AXES = ("gx_0", "gx_1", "gy_0", "gy_1")
GX = ("gx_0", "gx_1")
GY = ("gy_0", "gy_1")

VMEM = pl.BlockSpec(memory_space=pltpu.VMEM)
SMEM = pl.BlockSpec(memory_space=pltpu.SMEM)
FAR = pl.BlockSpec(memory_space=pltpu.HBM)
PARAMS = pltpu.CompilerParams(vmem_limit_bytes=16 * 1024 * 1024)
F32 = jnp.float32


def tile_iota(axis):
    return lax.broadcasted_iota(jnp.int32, (8, 128), axis)


def shaped(*shape):
    return jax.ShapeDtypeStruct(shape, F32)


def prepare_kernel(parity, far_class, far_side, far_material, far_boundary, own, first, second, masked, *scratch):
    class_scale, right_side, material, boundary, sems = scratch
    copies = [
        pltpu.make_async_copy(far_class, class_scale, sems.at[3]),
        pltpu.make_async_copy(far_material, material, sems.at[0]),
        pltpu.make_async_copy(far_boundary, boundary, sems.at[1]),
        pltpu.make_async_copy(far_side, right_side, sems.at[2]),
    ]
    for copy in copies:
        copy.start()
    for copy in copies[:3]:
        copy.wait()
    even = parity[0] != 0.0
    for half in range(2):
        rows = pl.ds(half * 8, 8)
        fields = []
        for x in range(2):
            field = jnp.zeros((8, 128), F32)
            kinds = material[x, rows]
            for number in range(8):
                field = field + jnp.where(kinds == number, class_scale[number], 0.0)
            field = jnp.where(boundary[x, rows] == 1, 0.0, field)
            masked[x, rows] = field
            fields.append(field)
        first[pl.ds(384 + half * 8, 8)] = jnp.where(even, fields[1], fields[0])
        second[pl.ds(384 + half * 8, 8)] = jnp.where(even, fields[0], fields[1])

    copies[3].wait()

    def one_row(y, carry):
        for c in range(3):
            tile = jnp.concatenate([right_side[0, y, c], right_side[1, y, c]], axis=0)
            own[y, c] = tile
            first[pl.ds((y * 3 + c) * 8, 8)] = tile
            second[pl.ds((y * 3 + c) * 8, 8)] = tile
        return carry

    lax.fori_loop(0, 16, one_row, 0)


def prepare(parity, *operands):
    return pl.pallas_call(
        prepare_kernel,
        out_shape=(shaped(16, 3, 8, 128), shaped(400, 128), shaped(400, 128), shaped(2, 16, 128)),
        in_specs=[VMEM, FAR, FAR, FAR, FAR],
        out_specs=(VMEM,) * 4,
        scratch_shapes=[
            pltpu.SMEM((8,), F32),
            pltpu.VMEM((2, 16, 3, 4, 128), F32),
            pltpu.VMEM((2, 16, 128), jnp.int32),
            pltpu.VMEM((2, 16, 128), jnp.int32),
            pltpu.SemaphoreType.DMA((4,)),
        ],
        compiler_params=PARAMS,
        name="prepare",
    )(parity, *[pltpu.with_memory_space_constraint(x, pltpu.HBM) for x in operands])


def setup_kernel(stencil, class_scale, coef, interval):
    def fill(n, total):
        for k in range(9):
            tile = jnp.full((8, 128), stencil[n * 9 + k])
            coef[n * 9 + k] = tile
            total = total + tile * tile
        return total

    total = lax.fori_loop(0, 27, fill, jnp.zeros((8, 128), F32))
    centre = [jnp.full((8, 128), stencil[13 * 9 + n]) for n in (0, 4, 8)]
    middle = (centre[0] + centre[1] + centre[2]) / 3.0
    for tile in centre:
        total = total - tile * tile
    spread = jnp.sqrt(jnp.maximum(total, 0.0) / 3.0)
    least = most = jnp.full((8, 128), class_scale[0])
    for number in range(1, 8):
        value = jnp.full((8, 128), class_scale[number])
        least, most = jnp.minimum(least, value), jnp.maximum(most, value)
    bottom = jnp.minimum(least * (middle - spread), 1.0)
    top = jnp.maximum(most * (middle + spread), 1.0)
    shift = 0.5 * (bottom + top)
    interval[0] = shift
    interval[1] = jnp.maximum(0.5 * (top - bottom), 0.05 * shift)


def setup(stencil, class_scale):
    return pl.pallas_call(
        setup_kernel,
        out_shape=(shaped(243, 8, 128), shaped(2, 8, 128)),
        in_specs=[SMEM, SMEM],
        out_specs=(VMEM,) * 2,
        compiler_params=PARAMS,
        name="setup",
    )(stencil, class_scale)


def signs_kernel(rows, sign_bits, signs):
    lanes = lax.broadcasted_iota(jnp.int32, (1, 128), 1)
    size = 1.0 / math.sqrt(128.0)

    def sample(n, carry):
        for part in range(2):
            spot = rows[n + 64 * part]
            tile = lax.shift_right_logical(spot, 7)
            x = (tile >= 48).astype(jnp.int32)
            place = tile - 48 * x
            y = lax.shift_right_logical(place * 171, 9)
            bits = sign_bits[x, place - 3 * y, pl.ds(y, 1), :]
            common = (spot & 127) & lanes
            for by in (4, 2, 1):
                common = common ^ lax.shift_right_logical(common, by)
            row = jnp.where(((common ^ bits) & 1) == 1, size, -size)
            signs[n, pl.ds(4 * part, 4), :] = jnp.broadcast_to(row, (4, 128))
        return carry

    lax.fori_loop(0, 64, sample, 0, unroll=8)


def sample_signs(rows, sign_bits):
    return pl.pallas_call(
        signs_kernel,
        out_shape=shaped(64, 8, 128),
        in_specs=[SMEM, VMEM],
        out_specs=VMEM,
        compiler_params=PARAMS,
        name="signs",
    )(rows, sign_bits)


def stencil_rows(coef, component, rows, terms):
    sums = [[None] * rows for _ in range(3)]
    for dx, tile in terms:
        for c in range(3):
            tiles = [tile(r, c) for r in range(rows + 2)]
            for dy in range(3):
                for dz in range(3):
                    weight = coef[(dx * 9 + dy * 3 + dz) * 9 + component * 3 + c]
                    for r in range(rows):
                        term = weight * tiles[r + dy]
                        old = sums[dz][r]
                        sums[dz][r] = term if old is None else old + term
    lane = tile_iota(1)
    out = []
    for r in range(rows):
        low = jnp.where(lane > 0, pltpu.roll(sums[0][r], 1, 1), 0.0)
        high = jnp.where(lane < 127, pltpu.roll(sums[2][r], 127, 1), 0.0)
        out.append(sums[1][r] + low + high)
    return out


def five_pairs(put, left, own, right):
    half = tile_iota(0) < 4
    turned = [pltpu.roll(tile, 4, 0) for tile in (left, own, right)]
    put(0, left)
    put(1, jnp.where(half, turned[0], turned[1]))
    put(2, own)
    put(3, jnp.where(half, turned[1], turned[2]))
    put(4, right)


def recurrence(interval):
    shift = interval[0]
    gain = 2.0 / interval[1]
    inside, fixed = -shift * gain, gain - shift * gain

    def value(alpha, total, centre):
        return (alpha * gain) * total + jnp.where(alpha == 0.0, fixed, inside) * centre

    return value


SEVEN = 7


def inner_kernel(coef, own, part, turned):
    def turn_rows(y, carry):
        for c in range(3):
            turned[y, c] = pltpu.roll(own[y, c], 4, 0)
        return carry

    lax.fori_loop(0, 16, turn_rows, 0)

    def body(i, carry):
        component, first = i % 3, i // 3 * SEVEN
        for n, (dx, source) in enumerate(((2, own), (1, turned), (0, own))):
            terms = [(dx, lambda r, c, source=source: source[first + r, c])]
            for r, total in enumerate(stencil_rows(coef, component, SEVEN, terms)):
                part[first + r, n, component] = total
        return carry

    lax.fori_loop(0, 6, body, 0)


def inner(coef, own):
    return pl.pallas_call(
        inner_kernel,
        out_shape=shaped(14, 3, 3, 8, 128),
        in_specs=[VMEM, VMEM],
        out_specs=VMEM,
        scratch_shapes=[pltpu.VMEM((16, 3, 8, 128), F32)],
        compiler_params=PARAMS,
        name="inner",
    )(coef, own)


def second_step(mid, own, scale_own, value_of, coef, component, first, rows, last):
    terms = [(dx, lambda r, c, dx=dx: mid[first + r, dx, c]) for dx in range(3)]
    for r, total in enumerate(stencil_rows(coef, component, rows, terms)):
        row = first + r
        value = value_of(scale_own[row], total, mid[row + 1, 1, component])
        last[row, component] = value - own[row, component]


def join(mid, row):
    half = tile_iota(0) < 4
    for c in range(3):
        mid[row, 1, c] = jnp.where(
            half, pltpu.roll(mid[row, 0, c], 4, 0), pltpu.roll(mid[row, 2, c], 4, 0)
        )


def make_middle_kernel(first_round):
    def kernel(
        coef, interval, parity, swap_a, own, swap_b, part, before, scale, scale_own, mid, last,
        left, right, beside,
    ):
        half = tile_iota(0) < 4
        even = parity[0] != 0.0

        def fill(y, carry):
            for c in range(3):
                a, b = swap_a[y, c], swap_b[y, c]
                lower, upper = jnp.where(even, b, a), jnp.where(even, a, b)
                left[y, c] = lower
                right[y, c] = upper
                beside[y, c] = pltpu.roll(jnp.where(half, upper, lower), 4, 0)
            return carry

        lax.fori_loop(0, 16, fill, 0)
        value_of = recurrence(interval)

        def body(i, carry):
            component, first = i % 3, i // 3 * SEVEN
            sums = []
            for dx, source in ((0, left), (1, beside), (2, right)):
                terms = [(dx, lambda r, c, source=source: source[first + r, c])]
                sums.append(stencil_rows(coef, component, SEVEN, terms))
            for r in range(SEVEN):
                row = first + r
                near, far = part[row, 1, component], sums[1][r]
                turned = pltpu.roll(own[row + 1, component], 4, 0)
                centre = beside[row + 1, component]
                for side in range(2):
                    pick = half if side == 0 else jnp.logical_not(half)
                    total = sums[2 * side][r] + part[row, 2 * side, component]
                    value = value_of(
                        scale[row + 1, side],
                        total + jnp.where(pick, far, near),
                        jnp.where(pick, centre, turned),
                    )
                    if first_round:
                        value = value * 0.5
                    else:
                        value = value - before[row + 2, side * 2, component]
                    mid[row + 2, side * 2, component] = value
            return carry

        lax.fori_loop(0, 6, body, 0)

        def join_rows(row, carry):
            join(mid, row + 2)
            return carry

        lax.fori_loop(0, 14, join_rows, 0)

        def second(i, carry):
            second_step(mid, own, scale_own, value_of, coef, i % 3, 2 + i // 3 * 6, 6, last)
            return carry

        lax.fori_loop(0, 6, second, 0)

    return kernel


def middle(first_round, *operands):
    return pl.pallas_call(
        make_middle_kernel(first_round),
        out_shape=(shaped(18, 3, 3, 8, 128), shaped(16, 3, 8, 128)),
        in_specs=[VMEM] * 10,
        out_specs=(VMEM, VMEM),
        scratch_shapes=[pltpu.VMEM((16, 3, 8, 128), F32)] * 3,
        compiler_params=PARAMS,
        name="middle",
    )(*operands)


def make_outer_kernel(first_round, extra):
    final = extra > 0

    def kernel(
        coef, interval, parity, swap_a, own, swap_b, swap_c, swap_d, before, scale, scale_own,
        scale_far, mid_before, last_before, *refs,
    ):
        del mid_before, last_before
        if final:
            rows, signs, *parts = refs[:extra]
            table, both = refs[extra + 2], refs[-1]
        mid, last, *rest = refs[extra:]
        edge_scale, work = rest[-3:-1] if final else rest[-2:]
        value_of = recurrence(interval)
        even_x, even_y = parity[0] != 0.0, parity[1] != 0.0

        def message(n, row, c):
            if not first_round:
                return swap_c[n, row, c], swap_d[n, row, c]
            spot = pl.ds(((n * 2 + row) * 3 + c) * 8, 8)
            return swap_c[spot], swap_d[spot]

        for edge in range(2):
            for row in range(4):
                for c in range(3):

                    def put(n, tile):
                        work[edge, row, n, c] = tile

                    if (row < 2) == (edge == 0):
                        tiles = []
                        for n in range(3):
                            a, b = message(n, row % 2, c)
                            tiles.append(jnp.where(even_y, a, b) if edge else jnp.where(even_y, b, a))
                        five_pairs(put, *tiles)
                    else:
                        near = row - 2 if edge == 0 else row + 14
                        a, b = swap_a[near, c], swap_b[near, c]
                        five_pairs(
                            put, jnp.where(even_x, b, a), own[near, c], jnp.where(even_x, a, b)
                        )
            for side in range(2):
                if first_round:
                    planes = []
                    for x in range(2):
                        spot = pl.ds(144 + 2 * side + x, 1)
                        a, b = swap_c[spot], swap_d[spot]
                        row = jnp.where(even_y[0:1], a, b) if edge else jnp.where(even_y[0:1], b, a)
                        planes.append(jnp.broadcast_to(row, (8, 128)))
                    far_tile = jnp.where(tile_iota(0) < 4, planes[0], planes[1])
                    rest[0][edge, side] = far_tile
                else:
                    far_tile = scale_far[edge, side]
                edge_scale[edge, edge, side] = far_tile
                edge_scale[edge, 1 - edge, side] = scale[15 * edge, side]

        def edges(i, carry):
            edge, side = i // 2, i % 2
            terms = [(dx, lambda r, c, dx=dx: work[edge, r, side * 2 + dx, c]) for dx in range(3)]
            for component in range(3):
                for r, total in enumerate(stencil_rows(coef, component, 2, terms)):
                    row = edge * 16 + r
                    value = value_of(
                        edge_scale[edge, r, side], total, work[edge, r + 1, side * 2 + 1, component]
                    )
                    if first_round:
                        value = value * 0.5
                    else:
                        value = value - before[row, side * 2, component]
                    mid[row, side * 2, component] = value
            return carry

        lax.fori_loop(0, 4, edges, 0)
        for row in (0, 1, 16, 17):
            join(mid, row)

        def second(edge, carry):
            for component in range(3):
                second_step(mid, own, scale_own, value_of, coef, component, edge * 14, 2, last)
            return carry

        lax.fori_loop(0, 2, second, 0)
        if final:
            sketch_blocks(((mid, 1), (last, 0)), rows, signs, both, table, parts)

    return kernel


def outer(first_round, *operands, tail=()):
    extra = ()
    scratch = [pltpu.VMEM((2, 2, 2, 8, 128), F32), pltpu.VMEM((2, 4, 5, 3, 8, 128), F32)]
    if first_round:
        extra = (shaped(2, 2, 8, 128),)
    if tail:
        extra = (shaped(36, 128),)
        scratch.append(pltpu.VMEM((2, 96, 8, 128), F32))
    return pl.pallas_call(
        make_outer_kernel(first_round, len(tail)),
        out_shape=(shaped(18, 3, 3, 8, 128), shaped(16, 3, 8, 128), *extra),
        in_specs=[VMEM] * 14 + [SMEM] * bool(tail) + [VMEM] * (len(tail) - 1),
        out_specs=(VMEM,) * (2 + len(extra)),
        scratch_shapes=scratch,
        input_output_aliases={12: 0, 13: 1},
        compiler_params=PARAMS,
        name="outer",
    )(*operands, *tail)


def sketch_blocks(blocks, rows, signs, both, out, earlier=()):
    base = 0
    for part in earlier:
        size = part.shape[0]
        out[pl.ds(base, size), :] = part[...]
        base += size
    half = tile_iota(0) < 4
    lane = tile_iota(1)

    def spread(y, carry):
        for n, (block, kind) in enumerate(blocks):
            for c in range(3):
                tile = block[y + 1, 1, c] if kind else block[y, c]
                both[n, y * 3 + c] = tile
                both[n, 48 + y * 3 + c] = pltpu.roll(tile, 4, 0)
        return carry

    lax.fori_loop(0, 16, spread, 0)
    sums = [jnp.zeros((8, 128), F32)] * len(blocks)
    for j in range(64):
        first = lax.shift_right_logical(rows[j], 7)
        second = lax.shift_right_logical(rows[64 + j], 7)
        second = jnp.where(second < 48, second + 48, second - 48)
        sign = signs[j]
        for n in range(len(blocks)):
            tile = jnp.where(half, both[n, first], both[n, second]) * sign
            sums[n] = jnp.where(lane == j, jnp.sum(tile, axis=1, keepdims=True), sums[n])
    for n, total in enumerate(sums):
        folded = jnp.where(lane < 64, total, pltpu.roll(pltpu.roll(total, 64, 1), 4, 0))
        out[pl.ds(base + n * 4, 4), :] = folded[0:4]


def make_sketch_kernel(kinds):
    def kernel(rows, signs, *refs):
        blocks = list(zip(refs[: len(kinds)], kinds))
        sketch_blocks(blocks, rows, signs, refs[-1], refs[-2])

    return kernel


def sketch(kinds, rows, signs, blocks):
    return pl.pallas_call(
        make_sketch_kernel(kinds),
        out_shape=shaped(4 * len(kinds), 128),
        in_specs=[SMEM] + [VMEM] * (1 + len(kinds)),
        out_specs=VMEM,
        scratch_shapes=[pltpu.VMEM((len(kinds), 96, 8, 128), F32)],
        compiler_params=PARAMS,
        name="sketch",
    )(rows, signs, *blocks)


def dot(a, b):
    return jnp.dot(a, b, precision=lax.Precision.HIGHEST, preferred_element_type=F32)


def sum_lanes(a):
    return jnp.sum(a, axis=1, keepdims=True)


def fit(table, shift, reach):
    lane = tile_iota(1)
    row = tile_iota(0)
    live = row < 4
    raise_by = jnp.where(lane < 4, reach, 0.5 * reach)
    lower_by = jnp.where(lane < 4, 0.0, 0.5 * reach)

    def move(coords):
        return (
            pltpu.roll(coords * raise_by, 4, 1)
            + shift * coords
            + pltpu.roll(coords * lower_by, 124, 1)
        )

    rhs = jnp.where(live, table[0:8], 0.0)
    norms = jnp.sqrt(sum_lanes(rhs * rhs) + 1e-06)
    basis = rhs / norms
    coords = jnp.where(live & (lane == row), 1.0, 0.0) / norms
    leading = jnp.sum(jnp.where(lane == row, coords, 0.0), axis=0, keepdims=True)
    for k in range(STEPS - 1):
        moved = move(coords)
        image = dot(moved[:, 0:40], table)
        rest, next_coords = image, moved
        for i in range(4):
            weight = sum_lanes(image * basis[i : i + 1])
            rest = rest - weight * basis[i : i + 1]
            next_coords = next_coords - weight * coords[i : i + 1]
        norms = jnp.sqrt(sum_lanes(rest * rest) + 1e-06)
        basis = rest / norms
        coords = next_coords / norms
        leading = leading + jnp.sum(
            jnp.where(live & (lane == row + 4 * (k + 1)), coords, 0.0), axis=0, keepdims=True
        )

    tall_row = lax.broadcasted_iota(jnp.int32, (40, 128), 0)
    tall_lane = lax.broadcasted_iota(jnp.int32, (40, 128), 1)
    wide = shift[0:1]
    part = 0.5 * reach[0:1]
    lower = jnp.concatenate([table[4:8], table[0:36]], axis=0)
    upper = jnp.concatenate([table[4:40], table[0:4]], axis=0)
    vectors = wide * table + part * (lower + upper)
    rhs_rows = jnp.concatenate([rhs, rhs, rhs, rhs, rhs], axis=0)
    vectors = jnp.where(tall_row < 32, vectors, rhs_rows)

    combos = jnp.where(tall_row == tall_lane, 1.0, 0.0)
    found = jnp.zeros((8, 128), F32)
    sizes = jnp.zeros((1, 128), F32)
    for j in range(4 * STEPS):
        pivot = vectors[j : j + 1]
        products = sum_lanes(vectors * pivot)
        size = products[j : j + 1]
        ratio = products / (size + 1e-37)
        found = jnp.where(lane == j, ratio[32:40], found)
        sizes = jnp.where(lane[0:1] == j, size, sizes)
        later = jnp.where(tall_row > j, ratio, 0.0)
        vectors = vectors - later * pivot
        combos = combos - later * combos[j : j + 1]
    scaled = sizes * leading * leading
    found = jnp.where(live, found * (scaled / (scaled + 1e-06)), 0.0)
    return move, dot(found[:, 0:40], combos)


def finish_kernel(table, interval, first, m0, l0, m1, l1, m2, l2, m3, l3, iterate, remainder, mix):
    shift, reach = interval[0], interval[1]
    lane = tile_iota(1)
    row = tile_iota(0)
    sub = row % 4
    total = table[0]
    for n in range(1, table.shape[0]):
        total = total + table[n]
    tall = jnp.concatenate([total, jnp.zeros((4, 128), F32)], axis=0)
    move, weights = fit(tall, shift, reach)
    weights = jnp.where(lane < 4 * STEPS, weights, 0.0)
    images = move(weights)
    weights = jnp.where(row < 4, weights, pltpu.roll(weights, 4, 0))
    images = jnp.where(row < 4, images, pltpu.roll(images, 4, 0))
    for k in range(STEPS + 1):
        for r in range(4):
            spot = lane == 4 * k + (sub + r) % 4
            if k < STEPS:
                mix[0, k * 4 + r] = jnp.broadcast_to(
                    sum_lanes(jnp.where(spot, weights, 0.0)), (8, 128)
                )
            mix[1, k * 4 + r] = jnp.broadcast_to(
                sum_lanes(jnp.where(spot, images, 0.0)), (8, 128)
            )

    refs = [(first, 0), (m0, 1), (l0, 0), (m1, 1), (l1, 0), (m2, 1), (l2, 0), (m3, 1), (l3, 0)]

    def one_row(y, carry):
        for c in range(3):
            total = None
            image = first[y, c]
            for k, (ref, kind) in enumerate(refs):
                tile = ref[y + 1, 1, c] if kind else ref[y, c]
                for r in range(4):
                    if r:
                        turned = jnp.where(
                            sub < 4 - r, pltpu.roll(tile, 8 - r, 0), pltpu.roll(tile, 4 - r, 0)
                        )
                    else:
                        turned = tile
                    if k < STEPS:
                        part = mix[0, k * 4 + r] * turned
                        total = part if total is None else total + part
                    image = image - mix[1, k * 4 + r] * turned
            for x in range(2):
                iterate[x, y, c] = total[4 * x : 4 * x + 4]
                remainder[x, y, c] = image[4 * x : 4 * x + 4]
        return carry

    lax.fori_loop(0, 16, one_row, 0)


def finish(table, interval, blocks):
    return pl.pallas_call(
        finish_kernel,
        out_shape=(shaped(2, 16, 3, 4, 128), shaped(2, 16, 3, 4, 128)),
        in_specs=[VMEM] * 11,
        out_specs=(VMEM, VMEM),
        scratch_shapes=[pltpu.VMEM((2, 36, 8, 128), F32)],
        compiler_params=PARAMS,
        name="finish",
    )(table, interval, *blocks)


def swap(first, second, axis):
    count = lax.axis_size(axis)
    out = []
    for start, operand in ((0, first), (1, second)):
        pairs = [(i + k, i + 1 - k) for i in range(start, count - 1, 2) for k in range(2)]
        out.append(lax.ppermute(operand, axis, pairs))
    return out


def fold(count, *operands):
    def kernel(*refs):
        tables = []
        for ref in refs[:-1]:
            tables += [ref[...]] if len(ref.shape) == 2 else [ref[n] for n in range(ref.shape[0])]
        total = tables[0]
        for table in tables[1:]:
            total = total + table
        for n in range(count):
            refs[-1][n] = total

    return pl.pallas_call(
        kernel,
        out_shape=shaped(count, 36, 128),
        in_specs=[VMEM] * len(operands),
        out_specs=VMEM,
        compiler_params=PARAMS,
        name="fold",
    )(*operands)


def cycle(right_side, stencil, class_scale, material, boundary, sign_bits, sample_rows):
    rows = sample_rows.reshape(-1)
    flags = [lax.axis_index(axis) % 2 == 0 for axis in (GX, GY)]
    parity = jnp.stack([jnp.broadcast_to(flag.astype(F32), (8, 128)) for flag in flags])
    own, first, second, masked = prepare(
        parity, class_scale, right_side.transpose(0, 1, 3, 2, 4), material, boundary
    )
    blocks = [own]
    sketches = []

    for turn in range(STEPS // 2):
        first_round = turn == 0
        if first_round:
            swap_a, swap_b = swap(first, second, GX)
            coef, interval = setup(stencil.reshape(-1), class_scale)
        else:
            swap_a, swap_b = swap(own, own, GX)
        if turn == 1:
            signs = sample_signs(rows, sign_bits.transpose(0, 2, 1, 3))
        if not first_round:
            kinds = (0, 1, 0) if turn == 1 else (1, 0)
            part = sketch(kinds, rows, signs, blocks[-len(kinds) :])
        started = inner(coef, own)
        if first_round:
            swap_a, swap_b, started, masked = lax.optimization_barrier(
                (swap_a, swap_b, started, masked)
            )
            planes = [swap_a[None, 384:], swap_b[None, 384:]]
            planes = jnp.concatenate(
                [
                    jnp.where(flags[0], planes[1], planes[0]),
                    masked,
                    jnp.where(flags[0], planes[0], planes[1]),
                ]
            )
            swap_a, swap_b = swap_a[:384].reshape(own.shape), swap_b[:384].reshape(own.shape)
        else:
            swap_a, swap_b, part, started = lax.optimization_barrier(
                (swap_a, swap_b, part, started)
            )
            sketches.append(part)

        def ends(first):
            a, b = swap_a[first : first + 2], swap_b[first : first + 2]
            return jnp.stack(
                [
                    jnp.where(flags[0], b, a),
                    own[first : first + 2],
                    jnp.where(flags[0], a, b),
                ]
            )

        bottom, top = ends(0), ends(14)
        if first_round:
            flat = (3 * 2 * 3 * 8, 128)
            bottom = jnp.concatenate([bottom.reshape(flat), planes[:, 0], planes[:, 0]])
            top = jnp.concatenate([top.reshape(flat), planes[:, 15], planes[:, 15]])
        swap_c, swap_d = swap(
            jnp.where(flags[1], top, bottom), jnp.where(flags[1], bottom, top), GY
        )
        if first_round:
            pairs = planes.reshape(2, 2, 16, 128).transpose(2, 0, 1, 3)
            scale = jnp.broadcast_to(pairs[:, :, :, None], (16, 2, 2, 4, 128))
            scale = scale.reshape(16, 2, 8, 128)
            scale_own = jnp.broadcast_to(
                masked.transpose(1, 0, 2)[:, :, None], (16, 2, 4, 128)
            ).reshape(16, 8, 128)
            before = scale_far = interval
        else:
            before = blocks[-2]
        shared = (coef, interval, parity, swap_a, own, swap_b)
        started = middle(first_round, *shared, started, before, scale, scale_own)
        done = outer(
            first_round,
            *shared,
            *(swap_c, swap_d, before, scale, scale_own, scale_far, *started),
            tail=(rows, signs, *sketches) if turn == STEPS // 2 - 1 else (),
        )
        if first_round:
            scale_far = done[2]
        own = done[1]
        blocks += done[:2]

    table = done[2]
    other = lax.ppermute(table, "gy_1", [(0, 1), (1, 0)])
    copies = lax.all_to_all(fold(16, table, other), ("gx_0", "gy_0"), 0, 0, tiled=True)
    copies = lax.all_to_all(fold(8, copies), ("gx_1",), 0, 0, tiled=True)
    iterate, remainder = finish(copies, interval, blocks)
    return iterate.transpose(0, 1, 3, 2, 4), remainder.transpose(0, 1, 3, 2, 4)


def solution(mesh):
    split = Mesh(mesh.devices.reshape(4, 8, 4, 2), AXES)
    return jax.shard_map(
        cycle,
        mesh=split,
        in_specs=(
            P(GX, GY, None, None, None),
            P(),
            P(),
            P(GX, GY, None),
            P(GX, GY, None),
            P(GX, GY, None, None),
            P(GX, GY, None),
        ),
        out_specs=(P(GX, GY, None, None, None), P(GX, GY, None, None, None)),
        check_vma=False,
    )
```

```python
import math

import jax
import jax.numpy as jnp
from jax import lax
from jax.experimental import pallas as pl
from jax.experimental.pallas import tpu as pltpu
from jax.sharding import Mesh
from jax.sharding import PartitionSpec as P

STEPS = 8
AXES = ("gx_0", "gx_1", "gx_2", "gy_0", "gy_1")
GX = ("gx_0", "gx_1", "gx_2")
GY = ("gy_0", "gy_1")

VMEM = pl.BlockSpec(memory_space=pltpu.VMEM)
SMEM = pl.BlockSpec(memory_space=pltpu.SMEM)
FAR = pl.BlockSpec(memory_space=pltpu.HBM)
PARAMS = pltpu.CompilerParams(vmem_limit_bytes=16 * 1024 * 1024)
F32 = jnp.float32


def tile_iota(axis):
    return lax.broadcasted_iota(jnp.int32, (8, 128), axis)


def shaped(*shape):
    return jax.ShapeDtypeStruct(shape, F32)


def prepare_kernel(parity, far_class, far_side, far_material, far_boundary, own, first, second, masked, *scratch):
    class_scale, right_side, material, boundary, sems = scratch
    copies = [
        pltpu.make_async_copy(far_class, class_scale, sems.at[3]),
        pltpu.make_async_copy(far_material, material, sems.at[0]),
        pltpu.make_async_copy(far_boundary, boundary, sems.at[1]),
        pltpu.make_async_copy(far_side, right_side, sems.at[2]),
    ]
    for copy in copies:
        copy.start()
    for copy in copies[:3]:
        copy.wait()
    even = parity[0] != 0.0
    for half in range(2):
        rows = pl.ds(half * 8, 8)
        fields = []
        for x in range(2):
            field = jnp.zeros((8, 128), F32)
            kinds = material[x, rows]
            for number in range(8):
                field = field + jnp.where(kinds == number, class_scale[number], 0.0)
            field = jnp.where(boundary[x, rows] == 1, 0.0, field)
            masked[x, rows] = field
            fields.append(field)
        first[pl.ds(384 + half * 8, 8)] = jnp.where(even, fields[1], fields[0])
        second[pl.ds(384 + half * 8, 8)] = jnp.where(even, fields[0], fields[1])

    copies[3].wait()

    def one_row(y, carry):
        for c in range(3):
            tile = jnp.concatenate([right_side[0, y, c], right_side[1, y, c]], axis=0)
            own[y, c] = tile
            first[pl.ds((y * 3 + c) * 8, 8)] = tile
            second[pl.ds((y * 3 + c) * 8, 8)] = tile
        return carry

    lax.fori_loop(0, 16, one_row, 0)


def prepare(parity, *operands):
    return pl.pallas_call(
        prepare_kernel,
        out_shape=(shaped(16, 3, 8, 128), shaped(400, 128), shaped(400, 128), shaped(2, 16, 128)),
        in_specs=[VMEM, FAR, FAR, FAR, FAR],
        out_specs=(VMEM,) * 4,
        scratch_shapes=[
            pltpu.SMEM((8,), F32),
            pltpu.VMEM((2, 16, 3, 4, 128), F32),
            pltpu.VMEM((2, 16, 128), jnp.int32),
            pltpu.VMEM((2, 16, 128), jnp.int32),
            pltpu.SemaphoreType.DMA((4,)),
        ],
        compiler_params=PARAMS,
        name="prepare",
    )(parity, *[pltpu.with_memory_space_constraint(x, pltpu.HBM) for x in operands])


def setup_kernel(stencil, class_scale, coef, interval):
    def fill(n, total):
        for k in range(9):
            tile = jnp.full((8, 128), stencil[n * 9 + k])
            coef[n * 9 + k] = tile
            total = total + tile * tile
        return total

    total = lax.fori_loop(0, 27, fill, jnp.zeros((8, 128), F32))
    centre = [jnp.full((8, 128), stencil[13 * 9 + n]) for n in (0, 4, 8)]
    middle = (centre[0] + centre[1] + centre[2]) / 3.0
    for tile in centre:
        total = total - tile * tile
    spread = jnp.sqrt(jnp.maximum(total, 0.0) / 3.0)
    least = most = jnp.full((8, 128), class_scale[0])
    for number in range(1, 8):
        value = jnp.full((8, 128), class_scale[number])
        least, most = jnp.minimum(least, value), jnp.maximum(most, value)
    bottom = jnp.minimum(least * (middle - spread), 1.0)
    top = jnp.maximum(most * (middle + spread), 1.0)
    shift = 0.5 * (bottom + top)
    interval[0] = shift
    interval[1] = jnp.maximum(0.5 * (top - bottom), 0.05 * shift)


def setup(stencil, class_scale):
    return pl.pallas_call(
        setup_kernel,
        out_shape=(shaped(243, 8, 128), shaped(2, 8, 128)),
        in_specs=[SMEM, SMEM],
        out_specs=(VMEM,) * 2,
        compiler_params=PARAMS,
        name="setup",
    )(stencil, class_scale)


def signs_kernel(rows, sign_bits, signs):
    lanes = lax.broadcasted_iota(jnp.int32, (1, 128), 1)
    size = 1.0 / math.sqrt(128.0)

    def sample(n, carry):
        for part in range(2):
            spot = rows[n + 64 * part]
            tile = lax.shift_right_logical(spot, 7)
            x = (tile >= 48).astype(jnp.int32)
            place = tile - 48 * x
            y = lax.shift_right_logical(place * 171, 9)
            bits = sign_bits[x, place - 3 * y, pl.ds(y, 1), :]
            common = (spot & 127) & lanes
            for by in (4, 2, 1):
                common = common ^ lax.shift_right_logical(common, by)
            row = jnp.where(((common ^ bits) & 1) == 1, size, -size)
            signs[n, pl.ds(4 * part, 4), :] = jnp.broadcast_to(row, (4, 128))
        return carry

    lax.fori_loop(0, 64, sample, 0, unroll=8)


def sample_signs(rows, sign_bits):
    return pl.pallas_call(
        signs_kernel,
        out_shape=shaped(64, 8, 128),
        in_specs=[SMEM, VMEM],
        out_specs=VMEM,
        compiler_params=PARAMS,
        name="signs",
    )(rows, sign_bits)


def stencil_rows(coef, component, rows, terms):
    sums = [[None] * rows for _ in range(3)]
    for dx, tile in terms:
        for c in range(3):
            tiles = [tile(r, c) for r in range(rows + 2)]
            for dy in range(3):
                for dz in range(3):
                    weight = coef[(dx * 9 + dy * 3 + dz) * 9 + component * 3 + c]
                    for r in range(rows):
                        term = weight * tiles[r + dy]
                        old = sums[dz][r]
                        sums[dz][r] = term if old is None else old + term
    lane = tile_iota(1)
    out = []
    for r in range(rows):
        low = jnp.where(lane > 0, pltpu.roll(sums[0][r], 1, 1), 0.0)
        high = jnp.where(lane < 127, pltpu.roll(sums[2][r], 127, 1), 0.0)
        out.append(sums[1][r] + low + high)
    return out


def five_pairs(put, left, own, right):
    half = tile_iota(0) < 4
    turned = [pltpu.roll(tile, 4, 0) for tile in (left, own, right)]
    put(0, left)
    put(1, jnp.where(half, turned[0], turned[1]))
    put(2, own)
    put(3, jnp.where(half, turned[1], turned[2]))
    put(4, right)


def recurrence(interval):
    shift = interval[0]
    gain = 2.0 / interval[1]
    inside, fixed = -shift * gain, gain - shift * gain

    def value(alpha, total, centre):
        return (alpha * gain) * total + jnp.where(alpha == 0.0, fixed, inside) * centre

    return value


SEVEN = 7


def inner_kernel(coef, own, part, turned):
    def turn_rows(y, carry):
        for c in range(3):
            turned[y, c] = pltpu.roll(own[y, c], 4, 0)
        return carry

    lax.fori_loop(0, 16, turn_rows, 0)

    def body(i, carry):
        component, first = i % 3, i // 3 * SEVEN
        for n, (dx, source) in enumerate(((2, own), (1, turned), (0, own))):
            terms = [(dx, lambda r, c, source=source: source[first + r, c])]
            for r, total in enumerate(stencil_rows(coef, component, SEVEN, terms)):
                part[first + r, n, component] = total
        return carry

    lax.fori_loop(0, 6, body, 0)


def inner(coef, own):
    return pl.pallas_call(
        inner_kernel,
        out_shape=shaped(14, 3, 3, 8, 128),
        in_specs=[VMEM, VMEM],
        out_specs=VMEM,
        scratch_shapes=[pltpu.VMEM((16, 3, 8, 128), F32)],
        compiler_params=PARAMS,
        name="inner",
    )(coef, own)


def second_step(mid, own, scale_own, value_of, coef, component, first, rows, last):
    terms = [(dx, lambda r, c, dx=dx: mid[first + r, dx, c]) for dx in range(3)]
    for r, total in enumerate(stencil_rows(coef, component, rows, terms)):
        row = first + r
        value = value_of(scale_own[row], total, mid[row + 1, 1, component])
        last[row, component] = value - own[row, component]


def join(mid, row):
    half = tile_iota(0) < 4
    for c in range(3):
        mid[row, 1, c] = jnp.where(
            half, pltpu.roll(mid[row, 0, c], 4, 0), pltpu.roll(mid[row, 2, c], 4, 0)
        )


def make_middle_kernel(first_round):
    def kernel(
        coef, interval, parity, swap_a, own, swap_b, part, before, scale, scale_own, mid, last,
        left, right, beside,
    ):
        half = tile_iota(0) < 4
        even = parity[0] != 0.0

        def fill(y, carry):
            for c in range(3):
                a, b = swap_a[y, c], swap_b[y, c]
                lower, upper = jnp.where(even, b, a), jnp.where(even, a, b)
                left[y, c] = lower
                right[y, c] = upper
                beside[y, c] = pltpu.roll(jnp.where(half, upper, lower), 4, 0)
            return carry

        lax.fori_loop(0, 16, fill, 0)
        value_of = recurrence(interval)

        def body(i, carry):
            component, first = i % 3, i // 3 * SEVEN
            sums = []
            for dx, source in ((0, left), (1, beside), (2, right)):
                terms = [(dx, lambda r, c, source=source: source[first + r, c])]
                sums.append(stencil_rows(coef, component, SEVEN, terms))
            for r in range(SEVEN):
                row = first + r
                near, far = part[row, 1, component], sums[1][r]
                turned = pltpu.roll(own[row + 1, component], 4, 0)
                centre = beside[row + 1, component]
                for side in range(2):
                    pick = half if side == 0 else jnp.logical_not(half)
                    total = sums[2 * side][r] + part[row, 2 * side, component]
                    value = value_of(
                        scale[row + 1, side],
                        total + jnp.where(pick, far, near),
                        jnp.where(pick, centre, turned),
                    )
                    if first_round:
                        value = value * 0.5
                    else:
                        value = value - before[row + 2, side * 2, component]
                    mid[row + 2, side * 2, component] = value
            return carry

        lax.fori_loop(0, 6, body, 0)

        def join_rows(row, carry):
            join(mid, row + 2)
            return carry

        lax.fori_loop(0, 14, join_rows, 0)

        def second(i, carry):
            second_step(mid, own, scale_own, value_of, coef, i % 3, 2 + i // 3 * 6, 6, last)
            return carry

        lax.fori_loop(0, 6, second, 0)

    return kernel


def middle(first_round, *operands):
    return pl.pallas_call(
        make_middle_kernel(first_round),
        out_shape=(shaped(18, 3, 3, 8, 128), shaped(16, 3, 8, 128)),
        in_specs=[VMEM] * 10,
        out_specs=(VMEM, VMEM),
        scratch_shapes=[pltpu.VMEM((16, 3, 8, 128), F32)] * 3,
        compiler_params=PARAMS,
        name="middle",
    )(*operands)


def make_outer_kernel(first_round, extra):
    final = extra > 0

    def kernel(
        coef, interval, parity, swap_a, own, swap_b, swap_c, swap_d, before, scale, scale_own,
        scale_far, mid_before, last_before, *refs,
    ):
        del mid_before, last_before
        if final:
            rows, signs, *parts = refs[:extra]
            table, both = refs[extra + 2], refs[-1]
        mid, last, *rest = refs[extra:]
        edge_scale, work = rest[-3:-1] if final else rest[-2:]
        value_of = recurrence(interval)
        even_x, even_y = parity[0] != 0.0, parity[1] != 0.0

        def message(n, row, c):
            if not first_round:
                return swap_c[n, row, c], swap_d[n, row, c]
            spot = pl.ds(((n * 2 + row) * 3 + c) * 8, 8)
            return swap_c[spot], swap_d[spot]

        for edge in range(2):
            for row in range(4):
                for c in range(3):

                    def put(n, tile):
                        work[edge, row, n, c] = tile

                    if (row < 2) == (edge == 0):
                        tiles = []
                        for n in range(3):
                            a, b = message(n, row % 2, c)
                            tiles.append(jnp.where(even_y, a, b) if edge else jnp.where(even_y, b, a))
                        five_pairs(put, *tiles)
                    else:
                        near = row - 2 if edge == 0 else row + 14
                        a, b = swap_a[near, c], swap_b[near, c]
                        five_pairs(
                            put, jnp.where(even_x, b, a), own[near, c], jnp.where(even_x, a, b)
                        )
            for side in range(2):
                if first_round:
                    planes = []
                    for x in range(2):
                        spot = pl.ds(144 + 2 * side + x, 1)
                        a, b = swap_c[spot], swap_d[spot]
                        row = jnp.where(even_y[0:1], a, b) if edge else jnp.where(even_y[0:1], b, a)
                        planes.append(jnp.broadcast_to(row, (8, 128)))
                    far_tile = jnp.where(tile_iota(0) < 4, planes[0], planes[1])
                    rest[0][edge, side] = far_tile
                else:
                    far_tile = scale_far[edge, side]
                edge_scale[edge, edge, side] = far_tile
                edge_scale[edge, 1 - edge, side] = scale[15 * edge, side]

        def edges(i, carry):
            edge, side = i // 2, i % 2
            terms = [(dx, lambda r, c, dx=dx: work[edge, r, side * 2 + dx, c]) for dx in range(3)]
            for component in range(3):
                for r, total in enumerate(stencil_rows(coef, component, 2, terms)):
                    row = edge * 16 + r
                    value = value_of(
                        edge_scale[edge, r, side], total, work[edge, r + 1, side * 2 + 1, component]
                    )
                    if first_round:
                        value = value * 0.5
                    else:
                        value = value - before[row, side * 2, component]
                    mid[row, side * 2, component] = value
            return carry

        lax.fori_loop(0, 4, edges, 0)
        for row in (0, 1, 16, 17):
            join(mid, row)

        def second(edge, carry):
            for component in range(3):
                second_step(mid, own, scale_own, value_of, coef, component, edge * 14, 2, last)
            return carry

        lax.fori_loop(0, 2, second, 0)
        if final:
            sketch_blocks(((mid, 1), (last, 0)), rows, signs, both, table, parts)

    return kernel


def outer(first_round, *operands, tail=()):
    extra = ()
    scratch = [pltpu.VMEM((2, 2, 2, 8, 128), F32), pltpu.VMEM((2, 4, 5, 3, 8, 128), F32)]
    if first_round:
        extra = (shaped(2, 2, 8, 128),)
    if tail:
        extra = (shaped(36, 128),)
        scratch.append(pltpu.VMEM((2, 96, 8, 128), F32))
    return pl.pallas_call(
        make_outer_kernel(first_round, len(tail)),
        out_shape=(shaped(18, 3, 3, 8, 128), shaped(16, 3, 8, 128), *extra),
        in_specs=[VMEM] * 14 + [SMEM] * bool(tail) + [VMEM] * (len(tail) - 1),
        out_specs=(VMEM,) * (2 + len(extra)),
        scratch_shapes=scratch,
        input_output_aliases={12: 0, 13: 1},
        compiler_params=PARAMS,
        name="outer",
    )(*operands, *tail)


def sketch_blocks(blocks, rows, signs, both, out, earlier=()):
    base = 0
    for part in earlier:
        size = part.shape[0]
        out[pl.ds(base, size), :] = part[...]
        base += size
    half = tile_iota(0) < 4
    lane = tile_iota(1)

    def spread(y, carry):
        for n, (block, kind) in enumerate(blocks):
            for c in range(3):
                tile = block[y + 1, 1, c] if kind else block[y, c]
                both[n, y * 3 + c] = tile
                both[n, 48 + y * 3 + c] = pltpu.roll(tile, 4, 0)
        return carry

    lax.fori_loop(0, 16, spread, 0)
    sums = [jnp.zeros((8, 128), F32)] * len(blocks)
    for j in range(64):
        first = lax.shift_right_logical(rows[j], 7)
        second = lax.shift_right_logical(rows[64 + j], 7)
        second = jnp.where(second < 48, second + 48, second - 48)
        sign = signs[j]
        for n in range(len(blocks)):
            tile = jnp.where(half, both[n, first], both[n, second]) * sign
            sums[n] = jnp.where(lane == j, jnp.sum(tile, axis=1, keepdims=True), sums[n])
    for n, total in enumerate(sums):
        folded = jnp.where(lane < 64, total, pltpu.roll(pltpu.roll(total, 64, 1), 4, 0))
        out[pl.ds(base + n * 4, 4), :] = folded[0:4]


def make_sketch_kernel(kinds):
    def kernel(rows, signs, *refs):
        blocks = list(zip(refs[: len(kinds)], kinds))
        sketch_blocks(blocks, rows, signs, refs[-1], refs[-2])

    return kernel


def sketch(kinds, rows, signs, blocks):
    return pl.pallas_call(
        make_sketch_kernel(kinds),
        out_shape=shaped(4 * len(kinds), 128),
        in_specs=[SMEM] + [VMEM] * (1 + len(kinds)),
        out_specs=VMEM,
        scratch_shapes=[pltpu.VMEM((len(kinds), 96, 8, 128), F32)],
        compiler_params=PARAMS,
        name="sketch",
    )(rows, signs, *blocks)


def dot(a, b):
    return jnp.dot(a, b, precision=lax.Precision.HIGHEST, preferred_element_type=F32)


def sum_lanes(a):
    return jnp.sum(a, axis=1, keepdims=True)


def fit(table, shift, reach):
    lane = tile_iota(1)
    row = tile_iota(0)
    live = row < 4
    raise_by = jnp.where(lane < 4, reach, 0.5 * reach)
    lower_by = jnp.where(lane < 4, 0.0, 0.5 * reach)

    def move(coords):
        return (
            pltpu.roll(coords * raise_by, 4, 1)
            + shift * coords
            + pltpu.roll(coords * lower_by, 124, 1)
        )

    rhs = jnp.where(live, table[0:8], 0.0)
    tall_row = lax.broadcasted_iota(jnp.int32, (40, 128), 0)
    tall_lane = lax.broadcasted_iota(jnp.int32, (40, 128), 1)
    lower = jnp.concatenate([table[4:8], table[0:36]], axis=0)
    upper = jnp.concatenate([table[4:40], table[0:4]], axis=0)
    vectors = shift[0:1] * table + (0.5 * reach[0:1]) * (lower + upper)
    rhs_rows = jnp.concatenate([rhs, rhs, rhs, rhs, rhs], axis=0)
    vectors = jnp.where(tall_row < 32, vectors, rhs_rows)

    image_table = jnp.where(tall_row < 32, vectors, 0.0)
    scaling = lax.rsqrt(sum_lanes(rhs * rhs) + 1e-06)
    basis = rhs * scaling
    coords = jnp.where(live & (lane == row), 1.0, 0.0) * scaling
    leading = jnp.sum(jnp.where(lane == row, coords, 0.0), axis=0, keepdims=True)
    for k in range(STEPS - 1):
        image = dot(coords[:, 0:40], image_table)
        rest, next_coords = image, move(coords)
        for i in range(4):
            weight = sum_lanes(image * basis[i : i + 1])
            rest = rest - weight * basis[i : i + 1]
            next_coords = next_coords - weight * coords[i : i + 1]
        scaling = lax.rsqrt(sum_lanes(rest * rest) + 1e-06)
        basis = rest * scaling
        coords = next_coords * scaling
        leading = leading + jnp.sum(
            jnp.where(live & (lane == row + 4 * (k + 1)), coords, 0.0), axis=0, keepdims=True
        )

    combos = jnp.where(tall_row == tall_lane, 1.0, 0.0)
    found = jnp.zeros((8, 128), F32)
    sizes = jnp.ones((1, 128), F32)
    for j in range(4 * STEPS):
        pivot = vectors[j : j + 1]
        products = sum_lanes(vectors * pivot)
        size = products[j : j + 1]
        ratio = products * (1.0 / (size + 1e-37))
        found = jnp.where(lane == j, ratio[32:40], found)
        sizes = jnp.where(lane[0:1] == j, size, sizes)
        tail = j // 8 * 8
        later = jnp.where(tall_row[tail:] > j, ratio[tail:], 0.0)
        rest = vectors[tail:] - later * pivot
        more = combos[tail:] - later * combos[j : j + 1]
        vectors = jnp.concatenate([vectors[:tail], rest], axis=0) if tail else rest
        combos = jnp.concatenate([combos[:tail], more], axis=0) if tail else more
    scaled = sizes * leading * leading
    shrink = scaled / (scaled + 1e-06)
    found = jnp.where(live & (lane < 4 * STEPS), found * shrink, 0.0)
    return move, dot(found[:, 0:40], combos)


def finish_kernel(table, interval, first, m0, l0, m1, l1, m2, l2, m3, l3, iterate, remainder, mix):
    shift, reach = interval[0], interval[1]
    lane = tile_iota(1)
    row = tile_iota(0)
    sub = row % 4
    total = table[0]
    for n in range(1, table.shape[0]):
        total = total + table[n]
    tall = jnp.concatenate([total, jnp.zeros((4, 128), F32)], axis=0)
    move, weights = fit(tall, shift, reach)
    weights = jnp.where(lane < 4 * STEPS, weights, 0.0)
    images = move(weights)
    weights = jnp.where(row < 4, weights, pltpu.roll(weights, 4, 0))
    images = jnp.where(row < 4, images, pltpu.roll(images, 4, 0))
    for k in range(STEPS + 1):
        for r in range(4):
            spot = lane == 4 * k + (sub + r) % 4
            if k < STEPS:
                mix[0, k * 4 + r] = jnp.broadcast_to(
                    sum_lanes(jnp.where(spot, weights, 0.0)), (8, 128)
                )
            mix[1, k * 4 + r] = jnp.broadcast_to(
                sum_lanes(jnp.where(spot, images, 0.0)), (8, 128)
            )

    refs = [(first, 0), (m0, 1), (l0, 0), (m1, 1), (l1, 0), (m2, 1), (l2, 0), (m3, 1), (l3, 0)]

    turns = [row - sub + (sub + r) % 4 for r in range(4)]

    def one_row(y, carry):
        for c in range(3):
            total = None
            image = first[y, c]
            for k, (ref, kind) in enumerate(refs):
                tile = ref[y + 1, 1, c] if kind else ref[y, c]
                for r in range(4):
                    turned = jnp.take_along_axis(tile, turns[r], axis=0) if r else tile
                    if k < STEPS:
                        part = mix[0, k * 4 + r] * turned
                        total = part if total is None else total + part
                    image = image - mix[1, k * 4 + r] * turned
            for x in range(2):
                iterate[x, y, c] = total[4 * x : 4 * x + 4]
                remainder[x, y, c] = image[4 * x : 4 * x + 4]
        return carry

    lax.fori_loop(0, 16, one_row, 0)


def finish(table, interval, blocks):
    return pl.pallas_call(
        finish_kernel,
        out_shape=(shaped(2, 16, 3, 4, 128), shaped(2, 16, 3, 4, 128)),
        in_specs=[VMEM] * 11,
        out_specs=(VMEM, VMEM),
        scratch_shapes=[pltpu.VMEM((2, 36, 8, 128), F32)],
        compiler_params=PARAMS,
        name="finish",
    )(table, interval, *blocks)


def swap(first, second, axis):
    count = lax.axis_size(axis)
    out = []
    for start, operand in ((0, first), (1, second)):
        pairs = [(i + k, i + 1 - k) for i in range(start, count - 1, 2) for k in range(2)]
        out.append(lax.ppermute(operand, axis, pairs))
    return out


def fold(count, *operands):
    def kernel(*refs):
        tables = []
        for ref in refs[:-1]:
            tables += [ref[...]] if len(ref.shape) == 2 else [ref[n] for n in range(ref.shape[0])]
        total = tables[0]
        for table in tables[1:]:
            total = total + table
        for n in range(count):
            refs[-1][n] = total

    return pl.pallas_call(
        kernel,
        out_shape=shaped(count, 36, 128),
        in_specs=[VMEM] * len(operands),
        out_specs=VMEM,
        compiler_params=PARAMS,
        name="fold",
    )(*operands)


def cycle(right_side, stencil, class_scale, material, boundary, sign_bits, sample_rows):
    rows = sample_rows.reshape(-1)
    flags = [lax.axis_index(axis) % 2 == 0 for axis in (GX, GY)]
    parity = jnp.stack([jnp.broadcast_to(flag.astype(F32), (8, 128)) for flag in flags])
    own, first, second, masked = prepare(
        parity, class_scale, right_side.transpose(0, 1, 3, 2, 4), material, boundary
    )
    blocks = [own]
    sketches = []

    for turn in range(STEPS // 2):
        first_round = turn == 0
        if first_round:
            swap_a, swap_b = swap(first, second, GX)
            coef, interval = setup(stencil.reshape(-1), class_scale)
        else:
            swap_a, swap_b = swap(own, own, GX)
        if turn == 1:
            signs = sample_signs(rows, sign_bits.transpose(0, 2, 1, 3))
        if not first_round:
            kinds = (0, 1, 0) if turn == 1 else (1, 0)
            part = sketch(kinds, rows, signs, blocks[-len(kinds) :])
        started = inner(coef, own)
        if first_round:
            swap_a, swap_b, started, masked = lax.optimization_barrier(
                (swap_a, swap_b, started, masked)
            )
            planes = [swap_a[None, 384:], swap_b[None, 384:]]
            planes = jnp.concatenate(
                [
                    jnp.where(flags[0], planes[1], planes[0]),
                    masked,
                    jnp.where(flags[0], planes[0], planes[1]),
                ]
            )
            swap_a, swap_b = swap_a[:384].reshape(own.shape), swap_b[:384].reshape(own.shape)
        else:
            swap_a, swap_b, part, started = lax.optimization_barrier(
                (swap_a, swap_b, part, started)
            )
            sketches.append(part)

        def ends(first):
            a, b = swap_a[first : first + 2], swap_b[first : first + 2]
            return jnp.stack(
                [
                    jnp.where(flags[0], b, a),
                    own[first : first + 2],
                    jnp.where(flags[0], a, b),
                ]
            )

        bottom, top = ends(0), ends(14)
        if first_round:
            flat = (3 * 2 * 3 * 8, 128)
            bottom = jnp.concatenate([bottom.reshape(flat), planes[:, 0], planes[:, 0]])
            top = jnp.concatenate([top.reshape(flat), planes[:, 15], planes[:, 15]])
        swap_c, swap_d = swap(
            jnp.where(flags[1], top, bottom), jnp.where(flags[1], bottom, top), GY
        )
        if first_round:
            pairs = planes.reshape(2, 2, 16, 128).transpose(2, 0, 1, 3)
            scale = jnp.broadcast_to(pairs[:, :, :, None], (16, 2, 2, 4, 128))
            scale = scale.reshape(16, 2, 8, 128)
            scale_own = jnp.broadcast_to(
                masked.transpose(1, 0, 2)[:, :, None], (16, 2, 4, 128)
            ).reshape(16, 8, 128)
            before = scale_far = interval
        else:
            before = blocks[-2]
        shared = (coef, interval, parity, swap_a, own, swap_b)
        started = middle(first_round, *shared, started, before, scale, scale_own)
        done = outer(
            first_round,
            *shared,
            *(swap_c, swap_d, before, scale, scale_own, scale_far, *started),
            tail=(rows, signs, *sketches) if turn == STEPS // 2 - 1 else (),
        )
        if first_round:
            scale_far = done[2]
        own = done[1]
        blocks += done[:2]

    table = done[2]
    for axis in ("gy_1", "gx_2"):
        other = lax.ppermute(table, axis, [(0, 1), (1, 0)])
        count = 1 if axis == "gy_1" else 16
        copies = fold(count, table, other)
        table = copies.reshape(table.shape) if count == 1 else copies
    copies = lax.all_to_all(table, ("gx_0", "gy_0"), 0, 0, tiled=True)
    copies = lax.all_to_all(fold(4, copies), ("gx_1",), 0, 0, tiled=True)
    iterate, remainder = finish(copies, interval, blocks)
    return iterate.transpose(0, 1, 3, 2, 4), remainder.transpose(0, 1, 3, 2, 4)


def solution(mesh):
    split = Mesh(mesh.devices.reshape(4, 4, 2, 4, 2), AXES)
    return jax.shard_map(
        cycle,
        mesh=split,
        in_specs=(
            P(GX, GY, None, None, None),
            P(),
            P(),
            P(GX, GY, None),
            P(GX, GY, None),
            P(GX, GY, None, None),
            P(GX, GY, None),
        ),
        out_specs=(P(GX, GY, None, None, None), P(GX, GY, None, None, None)),
        check_vma=False,
    )
```

```python
import math

import jax
import jax.numpy as jnp
from jax import lax
from jax.experimental import pallas as pl
from jax.experimental.pallas import tpu as pltpu
from jax.sharding import Mesh
from jax.sharding import PartitionSpec as P

STEPS = 8
AXES = ("gx_0", "gx_1", "gy_0", "gy_1")
GX = ("gx_0", "gx_1")
GY = ("gy_0", "gy_1")

VMEM = pl.BlockSpec(memory_space=pltpu.VMEM)
SMEM = pl.BlockSpec(memory_space=pltpu.SMEM)
FAR = pl.BlockSpec(memory_space=pltpu.HBM)
PARAMS = pltpu.CompilerParams(vmem_limit_bytes=16 * 1024 * 1024)
F32 = jnp.float32


def tile_iota(axis):
    return lax.broadcasted_iota(jnp.int32, (8, 128), axis)


def shaped(*shape):
    return jax.ShapeDtypeStruct(shape, F32)


def prepare_kernel(parity, far_class, far_side, far_material, far_boundary, own, first, second, masked, *scratch):
    class_scale, right_side, material, boundary, sems = scratch
    copies = [
        pltpu.make_async_copy(far_class, class_scale, sems.at[3]),
        pltpu.make_async_copy(far_material, material, sems.at[0]),
        pltpu.make_async_copy(far_boundary, boundary, sems.at[1]),
        pltpu.make_async_copy(far_side, right_side, sems.at[2]),
    ]
    for copy in copies:
        copy.start()
    for copy in copies[:3]:
        copy.wait()
    even = parity[0] != 0.0
    for half in range(2):
        rows = pl.ds(half * 8, 8)
        fields = []
        for x in range(2):
            field = jnp.zeros((8, 128), F32)
            kinds = material[x, rows]
            for number in range(8):
                field = field + jnp.where(kinds == number, class_scale[number], 0.0)
            field = jnp.where(boundary[x, rows] == 1, 0.0, field)
            masked[x, rows] = field
            fields.append(field)
        first[pl.ds(384 + half * 8, 8)] = jnp.where(even, fields[1], fields[0])
        second[pl.ds(384 + half * 8, 8)] = jnp.where(even, fields[0], fields[1])

    copies[3].wait()

    def one_row(y, carry):
        for c in range(3):
            tile = jnp.concatenate([right_side[0, y, c], right_side[1, y, c]], axis=0)
            own[y, c] = tile
            first[pl.ds((y * 3 + c) * 8, 8)] = tile
            second[pl.ds((y * 3 + c) * 8, 8)] = tile
        return carry

    lax.fori_loop(0, 16, one_row, 0)


def prepare(parity, *operands):
    return pl.pallas_call(
        prepare_kernel,
        out_shape=(shaped(16, 3, 8, 128), shaped(400, 128), shaped(400, 128), shaped(2, 16, 128)),
        in_specs=[VMEM, FAR, FAR, FAR, FAR],
        out_specs=(VMEM,) * 4,
        scratch_shapes=[
            pltpu.SMEM((8,), F32),
            pltpu.VMEM((2, 16, 3, 4, 128), F32),
            pltpu.VMEM((2, 16, 128), jnp.int32),
            pltpu.VMEM((2, 16, 128), jnp.int32),
            pltpu.SemaphoreType.DMA((4,)),
        ],
        compiler_params=PARAMS,
        name="prepare",
    )(parity, *[pltpu.with_memory_space_constraint(x, pltpu.HBM) for x in operands])


def setup_kernel(stencil, class_scale, coef, interval):
    def fill(n, total):
        for k in range(9):
            tile = jnp.full((8, 128), stencil[n * 9 + k])
            coef[n * 9 + k] = tile
            total = total + tile * tile
        return total

    total = lax.fori_loop(0, 27, fill, jnp.zeros((8, 128), F32))
    centre = [jnp.full((8, 128), stencil[13 * 9 + n]) for n in (0, 4, 8)]
    middle = (centre[0] + centre[1] + centre[2]) / 3.0
    for tile in centre:
        total = total - tile * tile
    spread = jnp.sqrt(jnp.maximum(total, 0.0) / 3.0)
    least = most = jnp.full((8, 128), class_scale[0])
    for number in range(1, 8):
        value = jnp.full((8, 128), class_scale[number])
        least, most = jnp.minimum(least, value), jnp.maximum(most, value)
    bottom = jnp.minimum(least * (middle - spread), 1.0)
    top = jnp.maximum(most * (middle + spread), 1.0)
    shift = 0.5 * (bottom + top)
    interval[0] = shift
    interval[1] = jnp.maximum(0.5 * (top - bottom), 0.05 * shift)


def setup(stencil, class_scale):
    return pl.pallas_call(
        setup_kernel,
        out_shape=(shaped(243, 8, 128), shaped(2, 8, 128)),
        in_specs=[SMEM, SMEM],
        out_specs=(VMEM,) * 2,
        compiler_params=PARAMS,
        name="setup",
    )(stencil, class_scale)


def signs_kernel(rows, sign_bits, signs):
    lanes = lax.broadcasted_iota(jnp.int32, (1, 128), 1)
    size = 1.0 / math.sqrt(128.0)

    def sample(n, carry):
        for part in range(2):
            spot = rows[n + 64 * part]
            tile = lax.shift_right_logical(spot, 7)
            x = (tile >= 48).astype(jnp.int32)
            place = tile - 48 * x
            y = lax.shift_right_logical(place * 171, 9)
            bits = sign_bits[x, place - 3 * y, pl.ds(y, 1), :]
            common = (spot & 127) & lanes
            for by in (4, 2, 1):
                common = common ^ lax.shift_right_logical(common, by)
            row = jnp.where(((common ^ bits) & 1) == 1, size, -size)
            signs[n, pl.ds(4 * part, 4), :] = jnp.broadcast_to(row, (4, 128))
        return carry

    lax.fori_loop(0, 64, sample, 0, unroll=8)


def sample_signs(rows, sign_bits):
    return pl.pallas_call(
        signs_kernel,
        out_shape=shaped(64, 8, 128),
        in_specs=[SMEM, VMEM],
        out_specs=VMEM,
        compiler_params=PARAMS,
        name="signs",
    )(rows, sign_bits)


def stencil_rows(coef, component, rows, terms):
    sums = [[None] * rows for _ in range(3)]
    for dx, tile in terms:
        for c in range(3):
            tiles = [tile(r, c) for r in range(rows + 2)]
            for dy in range(3):
                for dz in range(3):
                    weight = coef[(dx * 9 + dy * 3 + dz) * 9 + component * 3 + c]
                    for r in range(rows):
                        term = weight * tiles[r + dy]
                        old = sums[dz][r]
                        sums[dz][r] = term if old is None else old + term
    lane = tile_iota(1)
    out = []
    for r in range(rows):
        low = jnp.where(lane > 0, pltpu.roll(sums[0][r], 1, 1), 0.0)
        high = jnp.where(lane < 127, pltpu.roll(sums[2][r], 127, 1), 0.0)
        out.append(sums[1][r] + low + high)
    return out


def five_pairs(put, left, own, right):
    half = tile_iota(0) < 4
    turned = [pltpu.roll(tile, 4, 0) for tile in (left, own, right)]
    put(0, left)
    put(1, jnp.where(half, turned[0], turned[1]))
    put(2, own)
    put(3, jnp.where(half, turned[1], turned[2]))
    put(4, right)


def recurrence(interval):
    shift = interval[0]
    gain = 2.0 / interval[1]
    inside, fixed = -shift * gain, gain - shift * gain

    def value(alpha, total, centre):
        return (alpha * gain) * total + jnp.where(alpha == 0.0, fixed, inside) * centre

    return value


SEVEN = 7


def inner_kernel(coef, own, part, turned):
    def turn_rows(y, carry):
        for c in range(3):
            turned[y, c] = pltpu.roll(own[y, c], 4, 0)
        return carry

    lax.fori_loop(0, 16, turn_rows, 0)

    def body(i, carry):
        component, first = i % 3, i // 3 * SEVEN
        for n, (dx, source) in enumerate(((2, own), (1, turned), (0, own))):
            terms = [(dx, lambda r, c, source=source: source[first + r, c])]
            for r, total in enumerate(stencil_rows(coef, component, SEVEN, terms)):
                part[first + r, n, component] = total
        return carry

    lax.fori_loop(0, 6, body, 0)


def inner(coef, own):
    return pl.pallas_call(
        inner_kernel,
        out_shape=shaped(14, 3, 3, 8, 128),
        in_specs=[VMEM, VMEM],
        out_specs=VMEM,
        scratch_shapes=[pltpu.VMEM((16, 3, 8, 128), F32)],
        compiler_params=PARAMS,
        name="inner",
    )(coef, own)


def second_step(mid, own, scale_own, value_of, coef, component, first, rows, last):
    terms = [(dx, lambda r, c, dx=dx: mid[first + r, dx, c]) for dx in range(3)]
    for r, total in enumerate(stencil_rows(coef, component, rows, terms)):
        row = first + r
        value = value_of(scale_own[row], total, mid[row + 1, 1, component])
        last[row, component] = value - own[row, component]


def join(mid, row):
    half = tile_iota(0) < 4
    for c in range(3):
        mid[row, 1, c] = jnp.where(
            half, pltpu.roll(mid[row, 0, c], 4, 0), pltpu.roll(mid[row, 2, c], 4, 0)
        )


def make_middle_kernel(first_round):
    def kernel(
        coef, interval, parity, swap_a, own, swap_b, part, before, scale, scale_own, mid, last,
        left, right, beside,
    ):
        half = tile_iota(0) < 4
        even = parity[0] != 0.0

        def fill(y, carry):
            for c in range(3):
                a, b = swap_a[y, c], swap_b[y, c]
                lower, upper = jnp.where(even, b, a), jnp.where(even, a, b)
                left[y, c] = lower
                right[y, c] = upper
                beside[y, c] = pltpu.roll(jnp.where(half, upper, lower), 4, 0)
            return carry

        lax.fori_loop(0, 16, fill, 0)
        value_of = recurrence(interval)

        def body(i, carry):
            component, first = i % 3, i // 3 * SEVEN
            sums = []
            for dx, source in ((0, left), (1, beside), (2, right)):
                terms = [(dx, lambda r, c, source=source: source[first + r, c])]
                sums.append(stencil_rows(coef, component, SEVEN, terms))
            for r in range(SEVEN):
                row = first + r
                near, far = part[row, 1, component], sums[1][r]
                turned = pltpu.roll(own[row + 1, component], 4, 0)
                centre = beside[row + 1, component]
                for side in range(2):
                    pick = half if side == 0 else jnp.logical_not(half)
                    total = sums[2 * side][r] + part[row, 2 * side, component]
                    value = value_of(
                        scale[row + 1, side],
                        total + jnp.where(pick, far, near),
                        jnp.where(pick, centre, turned),
                    )
                    if first_round:
                        value = value * 0.5
                    else:
                        value = value - before[row + 2, side * 2, component]
                    mid[row + 2, side * 2, component] = value
            return carry

        lax.fori_loop(0, 6, body, 0)

        def join_rows(row, carry):
            join(mid, row + 2)
            return carry

        lax.fori_loop(0, 14, join_rows, 0)

        def second(i, carry):
            second_step(mid, own, scale_own, value_of, coef, i % 3, 2 + i // 3 * 6, 6, last)
            return carry

        lax.fori_loop(0, 6, second, 0)

    return kernel


def middle(first_round, *operands):
    return pl.pallas_call(
        make_middle_kernel(first_round),
        out_shape=(shaped(18, 3, 3, 8, 128), shaped(16, 3, 8, 128)),
        in_specs=[VMEM] * 10,
        out_specs=(VMEM, VMEM),
        scratch_shapes=[pltpu.VMEM((16, 3, 8, 128), F32)] * 3,
        compiler_params=PARAMS,
        name="middle",
    )(*operands)


def make_outer_kernel(first_round, extra):
    final = extra > 0

    def kernel(
        coef, interval, parity, swap_a, own, swap_b, swap_c, swap_d, before, scale, scale_own,
        scale_far, mid_before, last_before, *refs,
    ):
        del mid_before, last_before
        if final:
            rows, signs, *parts = refs[:extra]
            table, both = refs[extra + 2], refs[-1]
        mid, last, *rest = refs[extra:]
        edge_scale, work = rest[-3:-1] if final else rest[-2:]
        value_of = recurrence(interval)
        even_x, even_y = parity[0] != 0.0, parity[1] != 0.0

        def message(n, row, c):
            if not first_round:
                return swap_c[n, row, c], swap_d[n, row, c]
            spot = pl.ds(((n * 2 + row) * 3 + c) * 8, 8)
            return swap_c[spot], swap_d[spot]

        for edge in range(2):
            for row in range(4):
                for c in range(3):

                    def put(n, tile):
                        work[edge, row, n, c] = tile

                    if (row < 2) == (edge == 0):
                        tiles = []
                        for n in range(3):
                            a, b = message(n, row % 2, c)
                            tiles.append(jnp.where(even_y, a, b) if edge else jnp.where(even_y, b, a))
                        five_pairs(put, *tiles)
                    else:
                        near = row - 2 if edge == 0 else row + 14
                        a, b = swap_a[near, c], swap_b[near, c]
                        five_pairs(
                            put, jnp.where(even_x, b, a), own[near, c], jnp.where(even_x, a, b)
                        )
            for side in range(2):
                if first_round:
                    planes = []
                    for x in range(2):
                        spot = pl.ds(144 + 2 * side + x, 1)
                        a, b = swap_c[spot], swap_d[spot]
                        row = jnp.where(even_y[0:1], a, b) if edge else jnp.where(even_y[0:1], b, a)
                        planes.append(jnp.broadcast_to(row, (8, 128)))
                    far_tile = jnp.where(tile_iota(0) < 4, planes[0], planes[1])
                    rest[0][edge, side] = far_tile
                else:
                    far_tile = scale_far[edge, side]
                edge_scale[edge, edge, side] = far_tile
                edge_scale[edge, 1 - edge, side] = scale[15 * edge, side]

        def edges(i, carry):
            edge, side = i // 2, i % 2
            terms = [(dx, lambda r, c, dx=dx: work[edge, r, side * 2 + dx, c]) for dx in range(3)]
            for component in range(3):
                for r, total in enumerate(stencil_rows(coef, component, 2, terms)):
                    row = edge * 16 + r
                    value = value_of(
                        edge_scale[edge, r, side], total, work[edge, r + 1, side * 2 + 1, component]
                    )
                    if first_round:
                        value = value * 0.5
                    else:
                        value = value - before[row, side * 2, component]
                    mid[row, side * 2, component] = value
            return carry

        lax.fori_loop(0, 4, edges, 0)
        for row in (0, 1, 16, 17):
            join(mid, row)

        def second(edge, carry):
            for component in range(3):
                second_step(mid, own, scale_own, value_of, coef, component, edge * 14, 2, last)
            return carry

        lax.fori_loop(0, 2, second, 0)
        if final:
            sketch_blocks(((mid, 1), (last, 0)), rows, signs, both, table, parts)

    return kernel


def outer(first_round, *operands, tail=()):
    extra = ()
    scratch = [pltpu.VMEM((2, 2, 2, 8, 128), F32), pltpu.VMEM((2, 4, 5, 3, 8, 128), F32)]
    if first_round:
        extra = (shaped(2, 2, 8, 128),)
    if tail:
        extra = (shaped(36, 128),)
        scratch.append(pltpu.VMEM((2, 96, 8, 128), F32))
    return pl.pallas_call(
        make_outer_kernel(first_round, len(tail)),
        out_shape=(shaped(18, 3, 3, 8, 128), shaped(16, 3, 8, 128), *extra),
        in_specs=[VMEM] * 14 + [SMEM] * bool(tail) + [VMEM] * (len(tail) - 1),
        out_specs=(VMEM,) * (2 + len(extra)),
        scratch_shapes=scratch,
        input_output_aliases={12: 0, 13: 1},
        compiler_params=PARAMS,
        name="outer",
    )(*operands, *tail)


def sketch_blocks(blocks, rows, signs, both, out, earlier=()):
    base = 0
    for part in earlier:
        size = part.shape[0]
        out[pl.ds(base, size), :] = part[...]
        base += size
    half = tile_iota(0) < 4
    lane = tile_iota(1)

    def spread(y, carry):
        for n, (block, kind) in enumerate(blocks):
            for c in range(3):
                tile = block[y + 1, 1, c] if kind else block[y, c]
                both[n, y * 3 + c] = tile
                both[n, 48 + y * 3 + c] = pltpu.roll(tile, 4, 0)
        return carry

    lax.fori_loop(0, 16, spread, 0)
    sums = [jnp.zeros((8, 128), F32)] * len(blocks)
    for j in range(64):
        first = lax.shift_right_logical(rows[j], 7)
        second = lax.shift_right_logical(rows[64 + j], 7)
        second = jnp.where(second < 48, second + 48, second - 48)
        sign = signs[j]
        for n in range(len(blocks)):
            tile = jnp.where(half, both[n, first], both[n, second]) * sign
            sums[n] = jnp.where(lane == j, jnp.sum(tile, axis=1, keepdims=True), sums[n])
    for n, total in enumerate(sums):
        folded = jnp.where(lane < 64, total, pltpu.roll(pltpu.roll(total, 64, 1), 4, 0))
        out[pl.ds(base + n * 4, 4), :] = folded[0:4]


def make_sketch_kernel(kinds):
    def kernel(rows, signs, *refs):
        blocks = list(zip(refs[: len(kinds)], kinds))
        sketch_blocks(blocks, rows, signs, refs[-1], refs[-2])

    return kernel


def sketch(kinds, rows, signs, blocks):
    return pl.pallas_call(
        make_sketch_kernel(kinds),
        out_shape=shaped(4 * len(kinds), 128),
        in_specs=[SMEM] + [VMEM] * (1 + len(kinds)),
        out_specs=VMEM,
        scratch_shapes=[pltpu.VMEM((len(kinds), 96, 8, 128), F32)],
        compiler_params=PARAMS,
        name="sketch",
    )(rows, signs, *blocks)


def dot(a, b):
    return jnp.dot(a, b, precision=lax.Precision.HIGHEST, preferred_element_type=F32)


def sum_lanes(a):
    return jnp.sum(a, axis=1, keepdims=True)


def fit(table, shift, reach):
    lane = tile_iota(1)
    row = tile_iota(0)
    live = row < 4
    raise_by = jnp.where(lane < 4, reach, 0.5 * reach)
    lower_by = jnp.where(lane < 4, 0.0, 0.5 * reach)

    def move(coords):
        return (
            pltpu.roll(coords * raise_by, 4, 1)
            + shift * coords
            + pltpu.roll(coords * lower_by, 124, 1)
        )

    rhs = jnp.where(live, table[0:8], 0.0)
    tall_row = lax.broadcasted_iota(jnp.int32, (40, 128), 0)
    tall_lane = lax.broadcasted_iota(jnp.int32, (40, 128), 1)
    lower = jnp.concatenate([table[4:8], table[0:36]], axis=0)
    upper = jnp.concatenate([table[4:40], table[0:4]], axis=0)
    vectors = shift[0:1] * table + (0.5 * reach[0:1]) * (lower + upper)
    rhs_rows = jnp.concatenate([rhs, rhs, rhs, rhs, rhs], axis=0)
    vectors = jnp.where(tall_row < 32, vectors, rhs_rows)

    image_table = jnp.where(tall_row < 32, vectors, 0.0)
    scaling = lax.rsqrt(sum_lanes(rhs * rhs) + 1e-06)
    basis = rhs * scaling
    coords = jnp.where(live & (lane == row), 1.0, 0.0) * scaling
    leading = jnp.sum(jnp.where(lane == row, coords, 0.0), axis=0, keepdims=True)
    for k in range(STEPS - 1):
        image = dot(coords[:, 0:40], image_table)
        rest, next_coords = image, move(coords)
        for i in range(4):
            weight = sum_lanes(image * basis[i : i + 1])
            rest = rest - weight * basis[i : i + 1]
            next_coords = next_coords - weight * coords[i : i + 1]
        scaling = lax.rsqrt(sum_lanes(rest * rest) + 1e-06)
        basis = rest * scaling
        coords = next_coords * scaling
        leading = leading + jnp.sum(
            jnp.where(live & (lane == row + 4 * (k + 1)), coords, 0.0), axis=0, keepdims=True
        )

    combos = jnp.where(tall_row == tall_lane, 1.0, 0.0)
    found = jnp.zeros((8, 128), F32)
    sizes = jnp.ones((1, 128), F32)
    for j in range(4 * STEPS):
        pivot = vectors[j : j + 1]
        products = sum_lanes(vectors * pivot)
        size = products[j : j + 1]
        ratio = products * (1.0 / (size + 1e-37))
        found = jnp.where(lane == j, ratio[32:40], found)
        sizes = jnp.where(lane[0:1] == j, size, sizes)
        tail = j // 8 * 8
        later = jnp.where(tall_row[tail:] > j, ratio[tail:], 0.0)
        rest = vectors[tail:] - later * pivot
        more = combos[tail:] - later * combos[j : j + 1]
        vectors = jnp.concatenate([vectors[:tail], rest], axis=0) if tail else rest
        combos = jnp.concatenate([combos[:tail], more], axis=0) if tail else more
    scaled = sizes * leading * leading
    shrink = scaled / (scaled + 1e-06)
    found = jnp.where(live & (lane < 4 * STEPS), found * shrink, 0.0)
    return move, dot(found[:, 0:40], combos)


def finish_kernel(table, interval, first, m0, l0, m1, l1, m2, l2, m3, l3, iterate, remainder, mix):
    shift, reach = interval[0], interval[1]
    lane = tile_iota(1)
    row = tile_iota(0)
    sub = row % 4
    total = table[0]
    for n in range(1, table.shape[0]):
        total = total + table[n]
    tall = jnp.concatenate([total, jnp.zeros((4, 128), F32)], axis=0)
    move, weights = fit(tall, shift, reach)
    weights = jnp.where(lane < 4 * STEPS, weights, 0.0)
    images = move(weights)
    weights = jnp.where(row < 4, weights, pltpu.roll(weights, 4, 0))
    images = jnp.where(row < 4, images, pltpu.roll(images, 4, 0))
    for k in range(STEPS + 1):
        for r in range(4):
            spot = lane == 4 * k + (sub + r) % 4
            if k < STEPS:
                mix[0, k * 4 + r] = jnp.broadcast_to(
                    sum_lanes(jnp.where(spot, weights, 0.0)), (8, 128)
                )
            mix[1, k * 4 + r] = jnp.broadcast_to(
                sum_lanes(jnp.where(spot, images, 0.0)), (8, 128)
            )

    refs = [(first, 0), (m0, 1), (l0, 0), (m1, 1), (l1, 0), (m2, 1), (l2, 0), (m3, 1), (l3, 0)]

    turns = [row - sub + (sub + r) % 4 for r in range(4)]

    def one_row(y, carry):
        for c in range(3):
            total = None
            image = first[y, c]
            for k, (ref, kind) in enumerate(refs):
                tile = ref[y + 1, 1, c] if kind else ref[y, c]
                for r in range(4):
                    turned = jnp.take_along_axis(tile, turns[r], axis=0) if r else tile
                    if k < STEPS:
                        part = mix[0, k * 4 + r] * turned
                        total = part if total is None else total + part
                    image = image - mix[1, k * 4 + r] * turned
            for x in range(2):
                iterate[x, y, c] = total[4 * x : 4 * x + 4]
                remainder[x, y, c] = image[4 * x : 4 * x + 4]
        return carry

    lax.fori_loop(0, 16, one_row, 0, unroll=2)


def finish(table, interval, blocks):
    return pl.pallas_call(
        finish_kernel,
        out_shape=(shaped(2, 16, 3, 4, 128), shaped(2, 16, 3, 4, 128)),
        in_specs=[VMEM] * 11,
        out_specs=(VMEM, VMEM),
        scratch_shapes=[pltpu.VMEM((2, 36, 8, 128), F32)],
        compiler_params=PARAMS,
        name="finish",
    )(table, interval, *blocks)


def swap(first, second, axis):
    count = lax.axis_size(axis)
    out = []
    for start, operand in ((0, first), (1, second)):
        pairs = [(i + k, i + 1 - k) for i in range(start, count - 1, 2) for k in range(2)]
        out.append(lax.ppermute(operand, axis, pairs))
    return out


def fold(count, *operands):
    def kernel(*refs):
        tables = []
        for ref in refs[:-1]:
            tables += [ref[...]] if len(ref.shape) == 2 else [ref[n] for n in range(ref.shape[0])]
        total = tables[0]
        for table in tables[1:]:
            total = total + table
        for n in range(count):
            refs[-1][n] = total

    return pl.pallas_call(
        kernel,
        out_shape=shaped(count, 36, 128),
        in_specs=[VMEM] * len(operands),
        out_specs=VMEM,
        compiler_params=PARAMS,
        name="fold",
    )(*operands)


def cycle(right_side, stencil, class_scale, material, boundary, sign_bits, sample_rows):
    rows = sample_rows.reshape(-1)
    flags = [lax.axis_index(axis) % 2 == 0 for axis in (GX, GY)]
    parity = jnp.stack([jnp.broadcast_to(flag.astype(F32), (8, 128)) for flag in flags])
    own, first, second, masked = prepare(
        parity, class_scale, right_side.transpose(0, 1, 3, 2, 4), material, boundary
    )
    blocks = [own]
    sketches = []

    for turn in range(STEPS // 2):
        first_round = turn == 0
        if first_round:
            swap_a, swap_b = swap(first, second, GX)
            coef, interval = setup(stencil.reshape(-1), class_scale)
        else:
            swap_a, swap_b = swap(own, own, GX)
        if turn == 1:
            signs = sample_signs(rows, sign_bits.transpose(0, 2, 1, 3))
        if not first_round:
            kinds = (0, 1, 0) if turn == 1 else (1, 0)
            part = sketch(kinds, rows, signs, blocks[-len(kinds) :])
        started = inner(coef, own)
        if first_round:
            swap_a, swap_b, started, masked = lax.optimization_barrier(
                (swap_a, swap_b, started, masked)
            )
            planes = [swap_a[None, 384:], swap_b[None, 384:]]
            planes = jnp.concatenate(
                [
                    jnp.where(flags[0], planes[1], planes[0]),
                    masked,
                    jnp.where(flags[0], planes[0], planes[1]),
                ]
            )
            swap_a, swap_b = swap_a[:384].reshape(own.shape), swap_b[:384].reshape(own.shape)
        else:
            swap_a, swap_b, part, started = lax.optimization_barrier(
                (swap_a, swap_b, part, started)
            )
            sketches.append(part)

        def ends(first):
            a, b = swap_a[first : first + 2], swap_b[first : first + 2]
            return jnp.stack(
                [
                    jnp.where(flags[0], b, a),
                    own[first : first + 2],
                    jnp.where(flags[0], a, b),
                ]
            )

        bottom, top = ends(0), ends(14)
        if first_round:
            flat = (3 * 2 * 3 * 8, 128)
            bottom = jnp.concatenate([bottom.reshape(flat), planes[:, 0], planes[:, 0]])
            top = jnp.concatenate([top.reshape(flat), planes[:, 15], planes[:, 15]])
        swap_c, swap_d = swap(
            jnp.where(flags[1], top, bottom), jnp.where(flags[1], bottom, top), GY
        )
        if first_round:
            pairs = planes.reshape(2, 2, 16, 128).transpose(2, 0, 1, 3)
            scale = jnp.broadcast_to(pairs[:, :, :, None], (16, 2, 2, 4, 128))
            scale = scale.reshape(16, 2, 8, 128)
            scale_own = jnp.broadcast_to(
                masked.transpose(1, 0, 2)[:, :, None], (16, 2, 4, 128)
            ).reshape(16, 8, 128)
            before = scale_far = interval
        else:
            before = blocks[-2]
        shared = (coef, interval, parity, swap_a, own, swap_b)
        started = middle(first_round, *shared, started, before, scale, scale_own)
        done = outer(
            first_round,
            *shared,
            *(swap_c, swap_d, before, scale, scale_own, scale_far, *started),
            tail=(rows, signs, *sketches) if turn == STEPS // 2 - 1 else (),
        )
        if first_round:
            scale_far = done[2]
        own = done[1]
        blocks += done[:2]

    table = done[2]
    stages = (
        ("gy_1", ((0, 1),)),
        ("gx_1", ((0, 1), (2, 3), (4, 5), (6, 7))),
        ("gx_1", ((1, 2), (3, 4), (5, 6), (7, 0))),
        ("gx_1", ((1, 6), (2, 5), (3, 0), (4, 7))),
    )
    for n, (axis, pairs) in enumerate(stages):
        both_ways = [pair for a, b in pairs for pair in ((a, b), (b, a))]
        other = lax.ppermute(table, axis, both_ways)
        table = fold(1, table, other)[0] if n < 3 else fold(16, table, other)
    copies = lax.all_to_all(table, ("gx_0", "gy_0"), 0, 0, tiled=True)
    iterate, remainder = finish(copies, interval, blocks)
    return iterate.transpose(0, 1, 3, 2, 4), remainder.transpose(0, 1, 3, 2, 4)


def solution(mesh):
    split = Mesh(mesh.devices.reshape(4, 8, 4, 2), AXES)
    return jax.shard_map(
        cycle,
        mesh=split,
        in_specs=(
            P(GX, GY, None, None, None),
            P(),
            P(),
            P(GX, GY, None),
            P(GX, GY, None),
            P(GX, GY, None, None),
            P(GX, GY, None),
        ),
        out_specs=(P(GX, GY, None, None, None), P(GX, GY, None, None, None)),
        check_vma=False,
    )
```
